256 devices in a mesh: gx: 8 (over x, core), gy: 4 (over y), gz: 8 (over z).
Axes of the slice: x: 4, y: 4, z: 8, core: 2. Of those that a mesh axis runs over, the one named last changes fastest.
Arguments:
- dual_rhs: float32 [8, 4, 8, 3, 300, 128], P('gx', 'gy', 'gz'), may hold values from -6 to 6
- local_flex: bfloat16 [8, 4, 8, 1800, 1800], P('gx', 'gy', 'gz'), as said below
- corner_coupling: bfloat16 [8, 4, 8, 24, 1800], P('gx', 'gy', 'gz'), may hold values from -0.375 to 0.375
- face_stiffness: bfloat16 [8, 4, 8, 6, 300, 300], P('gx', 'gy', 'gz'), as said below
- coarse_inverse: bfloat16 [441, 441], replicated, as said below
- corner_ids: int32 [8, 4, 8, 8], P('gx', 'gy', 'gz'), may hold values from -1 to 146, as said below
Outputs:
- multipliers: float32 [8, 4, 8, 3, 300, 128], P('gx', 'gy', 'gz')
- residual: float32 [8, 4, 8, 3, 300, 128], P('gx', 'gy', 'gz')
The draws below stay inside these ranges and needn't reach their ends.
Inputs may be any that keep to these rules, and one draw needn't show every extreme that they name: `local_flex`: each subdomain's matrix is symmetric positive definite. `face_stiffness`: each face block is symmetric positive definite. `coarse_inverse`: symmetric positive definite. `corner_ids`: entry k = 4 kx + 2 ky + kz of subdomain (i, j, l) is the number of the corner at lattice point (i + kx, j + ky, l + kz) when that point has all coordinates strictly between 0 and the subdomain counts, else -1; the 147 interior corners are numbered by a permutation, so subdomains sharing a corner name the same node.
All inputs are finite; a program needn't handle non-finite values.
Results may differ from the reference program's by a relative error of at most 0.04.
Values may be sent and summed in bfloat16 or wider, within the bound.
A program may use at most 64 MiB of HBM per device.

```python
import math
import jax
import jax.numpy as jnp
from jax import lax

P_SIZE = 300
R = 128
ITERS = 3
SX = 8
SY = 4
SZ = 8
Q = 1800
NNODE = 147
NC = 441


def spd_block(block_key, order, lowest, highest, spread):
    first, second = jax.random.split(block_key, 2)
    diagonal = jax.random.uniform(first, (order,), jnp.float32, lowest, highest)
    gaussian = jax.random.normal(second, (order, order), jnp.float32)
    matrix = (gaussian + gaussian.T) * (spread / math.sqrt(2.0 * order)) + jnp.diag(diagonal)
    return matrix


def draw_local_flex(key, part):
    base_key = jax.random.fold_in(key, 11)

    def one_block(block_index):
        return spd_block(jax.random.fold_in(base_key, block_index), Q, 0.7, 1.8, 0.28).astype(jnp.bfloat16)
    matrices = lax.map(one_block, jnp.arange(SX * SY * SZ))
    return matrices.reshape(SX, SY, SZ, Q, Q)


def draw_face_stiffness(key, part):
    base_key = jax.random.fold_in(key, 23)

    def one_block(block_index):
        return spd_block(jax.random.fold_in(base_key, block_index), P_SIZE, 1.0, 2.5, 0.4).astype(jnp.bfloat16)
    matrices = lax.map(one_block, jnp.arange(SX * SY * SZ * 6))
    return matrices.reshape(SX, SY, SZ, 6, P_SIZE, P_SIZE)


def draw_coarse_inverse(key, part):
    return spd_block(jax.random.fold_in(key, 37), NC, 0.6, 1.4, 0.24).astype(jnp.bfloat16)


def draw_corner_ids(key, part):
    numbering = jax.random.permutation(jax.random.fold_in(key, 53), NNODE).astype(jnp.int32)
    corner = jnp.arange(8, dtype=jnp.int32)
    point_x = jnp.arange(SX, dtype=jnp.int32)[:, None, None, None] + corner // 4
    point_y = jnp.arange(SY, dtype=jnp.int32)[None, :, None, None] + corner // 2 % 2
    point_z = jnp.arange(SZ, dtype=jnp.int32)[None, None, :, None] + corner % 2
    inside = (point_x >= 1) & (point_x <= SX - 1) & (point_y >= 1) & (point_y <= SY - 1) & (point_z >= 1) & (point_z <= SZ - 1)
    lattice_index = ((point_x - 1) * (SY - 1) + (point_y - 1)) * (SZ - 1) + (point_z - 1)
    lattice_index = jnp.where(inside, lattice_index, 0)
    return jnp.where(inside, numbering[lattice_index], -1).astype(jnp.int32)


def level_of(rng, shape, cuts, low, top_value):
    factor_of, own = 1.0, jax.random.fold_in(rng, 6)
    for dim, parts in cuts:
        steps = jnp.exp(jax.random.uniform(jax.random.fold_in(own, dim), (parts,), jnp.float32, low / len(cuts), top_value / len(cuts)))
        factor_of = factor_of * jnp.repeat(steps, shape[dim] // parts).reshape([-1 if axis == dim else 1 for axis in range(len(shape))])
    return factor_of


def normal_values(stream_key, shape, deviation, bound, shards=(), held_as=jnp.bfloat16):
    level = level_of(stream_key, shape, shards, -0.22, 0.18) if shards else 1.0
    entries = jax.random.normal(stream_key, shape, jnp.float32) * deviation * level
    return jnp.minimum(jnp.maximum(entries, -bound), bound).astype(held_as)


def setup_inputs(seed: int = 0) -> dict:
    streams_of = jax.random.split(jax.random.key(seed), 7)
    dual_rhs = normal_values(streams_of[0], (SX, SY, SZ, 3, P_SIZE, R), 1.0, 6.0, ((0, 8), (1, 4), (2, 8)), jnp.float32)
    local_flex = draw_local_flex(jax.random.fold_in(streams_of[6], 71), 0)
    corner_coupling = normal_values(streams_of[2], (SX, SY, SZ, 24, Q), (Q // 8) ** -0.5, 0.375, ((0, 8), (1, 4), (2, 8)))
    face_stiffness = draw_face_stiffness(jax.random.fold_in(streams_of[6], 71), 0)
    coarse_inverse = draw_coarse_inverse(jax.random.fold_in(streams_of[6], 71), 0)
    corner_ids = draw_corner_ids(jax.random.fold_in(streams_of[6], 71), 0)
    return {"dual_rhs": dual_rhs, "local_flex": local_flex, "corner_coupling": corner_coupling, "face_stiffness": face_stiffness, "coarse_inverse": coarse_inverse, "corner_ids": corner_ids}


def reference(dual_rhs, local_flex, corner_coupling, face_stiffness, coarse_inverse, corner_ids):
    block_count = SX * SY * SZ
    grid_x = jnp.broadcast_to(jnp.arange(SX)[:, None, None], (SX, SY, SZ))
    grid_y = jnp.broadcast_to(jnp.arange(SY)[None, :, None], (SX, SY, SZ))
    grid_z = jnp.broadcast_to(jnp.arange(SZ)[None, None, :], (SX, SY, SZ))
    face_mask = jnp.stack([grid_x > 0, grid_x < SX - 1, grid_y > 0, grid_y < SY - 1, grid_z > 0, grid_z < SZ - 1], axis=-1).astype(jnp.float32)
    expanded = face_mask[..., None, None]
    face_sign = jnp.array([-1.0, 1.0, -1.0, 1.0, -1.0, 1.0], jnp.float32)[:, None, None]

    def duplicate(owned):
        face_list = []
        for axis_pos in range(3):
            plus_face = owned[:, :, :, axis_pos]
            face_list.append(jnp.roll(plus_face, 1, axis=axis_pos))
            face_list.append(plus_face)
        return jnp.stack(face_list, axis=3) * expanded

    def face_jump(values):
        face_list = []
        for axis_pos in range(3):
            minus_face = values[:, :, :, 2 * axis_pos]
            plus_face = values[:, :, :, 2 * axis_pos + 1]
            face_list.append(jnp.roll(plus_face, 1, axis=axis_pos) - minus_face)
            face_list.append(plus_face - jnp.roll(minus_face, -1, axis=axis_pos))
        return jnp.stack(face_list, axis=3) * expanded

    def face_product(operands):
        return jnp.dot(operands[0], operands[1], preferred_element_type=jnp.float32)

    stiff_flat = face_stiffness.reshape(block_count * 6, P_SIZE, P_SIZE)

    def precondition(dual):
        halved = (0.5 * face_sign * dual).astype(jnp.bfloat16)
        products = lax.map(face_product, (stiff_flat, halved.reshape(block_count * 6, P_SIZE, R)))
        return 0.5 * face_jump(products.reshape(SX, SY, SZ, 6, P_SIZE, R))

    flex_flat = local_flex.reshape(block_count, Q, Q)
    coupling_flat = corner_coupling.reshape(block_count, 24, Q)
    coupling_wide = coupling_flat.astype(jnp.float32)
    id_rows = corner_ids.reshape(block_count, 8)
    dof_ids = jnp.where(id_rows[:, :, None] >= 0, 3 * id_rows[:, :, None] + jnp.arange(3, dtype=jnp.int32)[None, None, :], NC).astype(jnp.int32).reshape(block_count, 24)

    def local_solve(operands):
        flex_block, coupling_block, signed_block = operands
        return (jnp.dot(flex_block, signed_block, preferred_element_type=jnp.float32),
                jnp.dot(coupling_block, signed_block, preferred_element_type=jnp.float32))

    def dual_operator(direction):
        signed = (face_sign * direction).astype(jnp.bfloat16).reshape(block_count, Q, R)
        local_image, corner_part = lax.map(local_solve, (flex_flat, coupling_flat, signed))
        coarse_rhs = jax.ops.segment_sum(corner_part.reshape(block_count * 24, R), dof_ids.reshape(-1), num_segments=NC + 1)[:NC]
        coarse_sol = jnp.dot(coarse_inverse, coarse_rhs.astype(jnp.bfloat16), preferred_element_type=jnp.float32)
        padded = jnp.concatenate([coarse_sol, jnp.zeros((1, R), jnp.float32)], axis=0)
        corner_sol = padded[dof_ids]
        displaced = local_image + jnp.einsum("nkq,nkr->nqr", coupling_wide, corner_sol, precision=lax.Precision.HIGHEST)
        curvature = jnp.sum(signed.astype(jnp.float32) * displaced, axis=(0, 1))
        return face_jump(displaced.reshape(SX, SY, SZ, 6, P_SIZE, R)), curvature

    def inner(left, right):
        return jnp.sum(left[:, :, :, 1::2] * right[:, :, :, 1::2], axis=(0, 1, 2, 3, 4))

    residual = duplicate(dual_rhs)
    multiplier = jnp.zeros_like(residual)
    precond_res = precondition(residual)
    rho_now = inner(residual, precond_res)
    direction = precond_res
    for iteration in range(ITERS):
        image, curvature = dual_operator(direction)
        step_size = rho_now / curvature
        multiplier = multiplier + step_size * direction
        residual = residual - step_size * image
        if iteration + 1 < ITERS:
            precond_res = precondition(residual)
            rho_next = inner(residual, precond_res)
            direction = precond_res + (rho_next / rho_now) * direction
            rho_now = rho_next
    return multiplier[:, :, :, 1::2], residual[:, :, :, 1::2]
```

```python
import functools

import jax
import jax.numpy as jnp
import numpy as np
from jax import lax
from jax.experimental import pallas as pl
from jax.experimental.pallas import tpu as pltpu
from jax.sharding import PartitionSpec as P

ITERS = 3
MESH = pl.DeviceIdType.MESH
F32 = jnp.float32
BF16 = jnp.bfloat16


def up_to(value, step):
    return -(-value // step) * step


def iota(shape, dim):
    return lax.broadcasted_iota(jnp.int32, shape, dim)


def dot(left, right, contract=None):
    if contract is None:
        contract = (left.ndim - 1, 0)
    dims = (((contract[0],), (contract[1],)), ((), ()))
    return lax.dot_general(left, right, dims, preferred_element_type=F32)


class Sizes:
    def __init__(self, grid, face, cases, coarse):
        self.grid, self.face, self.cases, self.coarse = grid, face, cases, coarse
        self.dofs = 6 * face
        self.wide = up_to(self.dofs, 128)
        self.window = up_to(face + 127, 128)
        nx, ny, nz = grid
        self.plane = (nx - 1) * (ny - 1)
        self.block = up_to(3 * self.plane + 1, 16)
        self.names = up_to(self.plane, 16)
        self.level = self.block + self.names
        self.rows = up_to(self.block * (nz - 1), 128)
        self.lines = nx * ny
        self.chips = nx // 2 * ny


def plane_sums(sz):
    nx, ny, _ = sz.grid
    table = np.zeros((sz.level, sz.lines * 16), np.float32)
    for i in range(nx):
        for j in range(ny):
            for kx in range(2):
                for ky in range(2):
                    x, y = i + kx, j + ky
                    if not (1 <= x < nx and 1 <= y < ny):
                        continue
                    spot = (x - 1) * (ny - 1) + y - 1
                    first = (i * ny + j) * 16
                    for d in range(3):
                        table[d * sz.plane + spot, first + (kx * 2 + ky) * 3 + d] = 1
                    table[sz.block + spot, first + 12 + kx * 2 + ky] = 1
    return table


def corner_order():
    table = np.zeros((32, 24), np.float32)
    for kx in range(2):
        for ky in range(2):
            for kz in range(2):
                for d in range(3):
                    row = kz * 16 + (kx * 2 + ky) * 3 + d
                    table[row, 3 * (4 * kx + 2 * ky + kz) + d] = 1
    return table


def kernel(sz, ids, rhs_h, flex_h, coup_h, stiff_h, inv_h, sums_h, order_h,
           x_ref, res_ref,
           rhs, flex, coup, stiff, inv, sums, order,
           rhs_b, rhs_n, stiff_n, cs, cn, own_t, nb_t, wide_t, ksum,
           r, s, u, p, sg, sgb, loc, cpb, rxy, lev, hb, hn, bmat, ae, pm, pa,
           ss, sx, sy, sp,
           load_sem, i_send, k_recv, r_recv, c_recv,
           xy_send, xy_recv, z_send, z_recv, pp_send, pp_recv, h_send, h_recv,
           sx_send, sx_recv, sy_send, sy_recv, sp_send, sp_recv):
    nx, ny, nz = sz.grid
    face, dofs = sz.face, sz.dofs
    i, j, l = lax.axis_index("gx"), lax.axis_index("gy"), lax.axis_index("gz")
    core = lax.rem(i, 2)
    place = (i, j, l)
    partner = {"gx": i + 1 - 2 * core, "gy": j, "gz": l}

    def toward(f):
        axis, step = f // 2, f % 2
        size = sz.grid[axis]
        spot = list(place)
        spot[axis] = lax.rem(spot[axis] + (1 if step else size - 1), size)
        return dict(zip(("gx", "gy", "gz"), spot))

    def far(di, dj):
        return min(di, nx - di) / 2 + min(dj, ny - dj)

    spread = sorted(
        [(di, dj) for di in range(nx) for dj in range(ny) if di or dj],
        key=lambda t: -far(*t),
    )
    chips = [(di, dj) for di, dj in spread if di % 2 == 0]
    lanes = sorted(range(1, nz), key=lambda t: -min(t, nz - t))

    def across(di, dj):
        return {"gx": lax.rem(i + di, nx), "gy": lax.rem(j + dj, ny), "gz": l}

    def along(dl):
        return {"gx": i, "gy": j, "gz": lax.rem(l + dl, nz)}

    def remote(src, dst, send, recv, target):
        return pltpu.make_async_remote_copy(
            src_ref=src, dst_ref=dst, send_sem=send, recv_sem=recv,
            device_id=target, device_id_type=MESH,
        )

    loads = []
    for n, (src, dst) in enumerate(
        ((stiff_h, stiff), (rhs_h, rhs), (coup_h, coup), (order_h, order),
         (flex_h, flex), (sums_h, sums), (inv_h, inv))
    ):
        copy = pltpu.make_async_copy(src, dst, load_sem.at[n])
        copy.start()
        loads.append(copy)

    barrier = pltpu.get_barrier_semaphore()
    for di, dj in spread:
        pl.semaphore_signal(barrier, inc=1, device_id=across(di, dj), device_id_type=MESH)
    for dl in lanes:
        pl.semaphore_signal(barrier, inc=1, device_id=along(dl), device_id_type=MESH)

    loads[1].wait()
    for a in range(3):
        rhs_b[a] = rhs[a].astype(BF16)
    loads[0].wait()
    pl.semaphore_wait(barrier, len(spread) + len(lanes))

    sent = []

    def send(src, dst, send_sem, recv_sem, target):
        copy = remote(src, dst, send_sem, recv_sem, target)
        copy.start()
        return copy

    for a in range(3):
        sent.append(send(rhs_b.at[a], rhs_n.at[a], i_send.at[a], r_recv.at[a], toward(2 * a + 1)))
    for f in range(6):
        sent.append(send(stiff.at[f], stiff_n.at[f ^ 1], i_send.at[3 + f], k_recv.at[f ^ 1], toward(f)))

    loads[2].wait()
    loads[3].wait()
    cs[...] = jnp.zeros_like(cs)
    cs[:, 0:dofs] = dot(order[...], coup[...]).astype(BF16)
    sgb[...] = jnp.zeros_like(sgb)
    starts = [face * f // 128 * 128 for f in range(6)]
    for f in range(6):
        sent.append(
            send(cs.at[:, pl.ds(starts[f], sz.window)], cn.at[f ^ 1], i_send.at[9 + f],
                 c_recv.at[f ^ 1], toward(f))
        )
    pick_row, pick_col = iota((32, 128), 0), iota((32, 128), 1)
    pick_own = ((pick_col & 63) == pick_row).astype(F32).astype(BF16)
    pick_nb = -((pick_col & 63) == pick_row + 32).astype(F32).astype(BF16)
    own_t[...] = dot(cs[...], pick_own, (0, 0))

    g_rows = 7 * 32
    line = iota((g_rows, 128), 0)
    g, kz, e = line >> 5, (line >> 4) & 1, line & 15
    t = (e * 11) >> 5
    d, kx, ky = e - 3 * t, t >> 1, t & 1

    def shift(minus, plus):
        return (g == plus).astype(jnp.int32) - (g == minus).astype(jnp.int32)

    gx = i + kx + shift(1, 2)
    gy = j + ky + shift(3, 4)
    gz = l + kz + shift(5, 6)
    inside = (e < 12) & (gx >= 1) & (gx < nx) & (gy >= 1) & (gy < ny) & (gz >= 1) & (gz < nz)
    spot = jnp.where(
        inside, sz.block * (gz - 1) + sz.plane * d + (ny - 1) * (gx - 1) + gy - 1, -1
    )
    for k in range(sz.rows // 128):
        ae[sz.rows:sz.rows + g_rows, 128 * k:128 * k + 128] = (
            (iota((g_rows, 128), 1) + 128 * k == spot).astype(F32).astype(BF16)
        )

    masks = []
    for f in range(6):
        axis, step = f // 2, f % 2
        edge = place[axis] < sz.grid[axis] - 1 if step else place[axis] > 0
        masks.append(jnp.where(edge, 1.0, 0.0).astype(F32))
    signs = [-1.0, 1.0] * 3

    def precondition(f):
        u[f] = (0.25 * masks[f]) * dot(ksum[f], r[f].astype(BF16))

    for a in range(3):
        r[2 * a + 1] = rhs[a] * masks[2 * a + 1]
        sent[a].wait_recv()
        r[2 * a] = rhs_n[a].astype(F32) * masks[2 * a]
    for f in range(6):
        remote(stiff.at[f], stiff_n.at[f], i_send.at[3 + f], k_recv.at[f], toward(f)).wait_recv()
        ksum[f] = (stiff[f].astype(F32) + stiff_n[f].astype(F32)).astype(BF16)
        precondition(f)

    def total(count, piece, send_sem, recv_sem):
        return remote(piece, piece, send_sem, recv_sem, partner)

    alpha = beta = gamma_old = curve = None
    for it in range(ITERS):
        last = it + 1 == ITERS
        tall = sz.level if it == 0 else sz.block
        for f in range(6):
            sg[face * f:face * f + face, :] = signs[f] * u[f]
        sgb[0:dofs, :] = sg[...].astype(BF16)
        cp = dot(cs[...], sgb[...])
        if it == 0:
            name = jnp.full((32, sz.cases), ids[7], jnp.int32).astype(F32)
            cp = jnp.where(iota((32, sz.cases), 0) == 31, name, cp)
        low, high = cp[0:16].astype(BF16), cp[16:32].astype(BF16)
        cpb[it, 0] = low
        cpb[it, 1] = high
        slot = i * ny + j
        for di, dj in spread:
            target = across(di, dj)
            send(cpb.at[it, lax.rem(target["gx"], 2)], rxy.at[it, slot], xy_send.at[it],
                 xy_recv.at[it], target)
        rxy[it, slot] = jnp.where(core == 0, low.astype(F32), high.astype(F32)).astype(BF16)

        gamma = sum(jnp.sum(r[f] * u[f], axis=0, keepdims=True) for f in (1, 3, 5))
        if it:
            cross = sum(jnp.sum(s[f] * u[f], axis=0, keepdims=True) for f in (1, 3, 5))
        else:
            cross = jnp.zeros_like(gamma)
        if it == 0:
            loads[4].wait()
        loc[...] = dot(flex[...], sgb[0:dofs, :])
        for f in range(6):
            hb[it, f] = loc[face * f:face * f + face, :].astype(BF16)
        delta = jnp.sum(sgb[0:dofs, :].astype(F32) * loc[...], axis=0, keepdims=True)

        where = iota((8, sz.cases), 0)
        packed = jnp.where(where == 0, gamma, jnp.where(where == 1, cross, jnp.where(where == 2, delta, 0.0)))
        chip = i // 2 * ny + j
        ss[it, 0] = packed
        sx[it, chip] = packed
        for di, dj in chips:
            send(ss.at[it, 0], sx.at[it, chip], sx_send.at[it], sx_recv.at[it], across(di, dj))
        for f in range(6):
            send(hb.at[it, f], hn.at[it, f ^ 1], h_send.at[it], h_recv.at[it], toward(f))

        if it == 0:
            loads[5].wait()
        total(0, rxy.at[it, pl.ds(0, sz.lines - 1)], xy_send.at[it], xy_recv.at[it]).wait_recv()
        lev[it, core, l] = dot(sums[...], rxy[it].reshape(sz.lines * 16, sz.cases)).astype(BF16)
        for dl in lanes:
            piece = lev.at[it, core, l, pl.ds(0, tall)]
            send(piece, piece, z_send.at[it], z_recv.at[it], along(dl))

        total(0, sx.at[it, pl.ds(0, sz.chips - 1)], sx_send.at[it], sx_recv.at[it]).wait_recv()
        packed = jnp.sum(sx[it], axis=0)
        ss[it, 1] = packed
        sy[it, l] = packed
        for dl in lanes:
            send(ss.at[it, 1], sy.at[it, l], sy_send.at[it], sy_recv.at[it], along(dl))

        if it == 0:
            for f in range(6):
                remote(cs.at[:, pl.ds(starts[f], sz.window)], cn.at[f], i_send.at[9 + f],
                       c_recv.at[f], toward(f)).wait_recv()
                nb_t[...] = dot(cn[f], pick_nb, (0, 0))
                off = face * (f ^ 1) - starts[f ^ 1]
                wide_t[f] = (own_t[face * f:face * f + face, :] + nb_t[off:off + face, :]).astype(BF16)

        total(0, sy.at[it, pl.ds(0, nz - 1)], sy_send.at[it], sy_recv.at[it]).wait_recv()
        mine = jnp.sum(sy[it], axis=0)
        ss[it, 2] = mine
        send(ss.at[it, 2], sp.at[it], sp_send.at[it], sp_recv.at[it], partner)

        total(0, lev.at[it, 0, pl.ds(0, nz - 1), pl.ds(0, tall)], z_send.at[it], z_recv.at[it]).wait_recv()
        piece = lev.at[it, core, pl.ds(0, nz), pl.ds(0, tall)]
        send(piece, piece, pp_send.at[it], pp_recv.at[it], partner)
        total(0, piece, pp_send.at[it], pp_recv.at[it]).wait_recv()

        if it == 0:
            bmat[...] = jnp.zeros_like(bmat)
            small_r, small_c = iota((sz.block, sz.names), 0), iota((sz.block, sz.names), 1)
            part = (small_r >= sz.plane).astype(jnp.int32) + (small_r >= 2 * sz.plane).astype(jnp.int32)
            expand = ((small_c == small_r - sz.plane * part) & (small_r < 3 * sz.plane)).astype(F32).astype(BF16)
            rr = iota((sz.block, 128), 0)
            comp = (rr >= sz.plane).astype(jnp.int32) + (rr >= 2 * sz.plane).astype(jnp.int32)
            pm[...] = jnp.zeros_like(pm)
        for z in range(1, nz):
            here = pl.ds(sz.block * (z - 1), sz.block)
            level = (
                lev[it, 0, z, 0:sz.block].astype(F32) + lev[it, 1, z - 1, 0:sz.block].astype(F32)
            )
            bmat[here, :] = level.astype(BF16)
            if it == 0:
                names = (
                    lev[it, 0, z, sz.block:sz.level].astype(F32)
                    + lev[it, 1, z - 1, sz.block:sz.level].astype(F32)
                ).astype(BF16)
                col = 3.0 * dot(expand, names) + comp.astype(F32)
                col = jnp.where(rr < 3 * sz.plane, col, -1.0)
                for k in range(up_to(sz.coarse, 128) // 128):
                    width = min(128, sz.coarse - 128 * k)
                    at = (iota((sz.block, 128), 1) + 128 * k).astype(F32)
                    pm[here, 128 * k:128 * k + width] = (at == col).astype(F32).astype(BF16)[:, 0:width]
        if it == 0:
            loads[6].wait()
            pa[...] = dot(pm[...], inv[...]).astype(BF16)
            ae[0:sz.rows, :] = dot(pa[...], pm[...], (1, 1)).astype(BF16)
            ae[sz.rows:sz.rows + g_rows, :] = dot(ae[sz.rows:sz.rows + g_rows, :], ae[0:sz.rows, :]).astype(BF16)

        sol = dot(ae[...], bmat[...])
        coarse_part = jnp.sum(sol[0:sz.rows] * bmat[...].astype(F32), axis=0, keepdims=True)
        near = sol[sz.rows:]
        near_hi = near.astype(BF16)
        near_lo = (near - near_hi.astype(F32)).astype(BF16)

        total(0, sp.at[it], sp_send.at[it], sp_recv.at[it]).wait_recv()
        sums_now = mine + sp[it]
        gamma, cross, delta = sums_now[0:1], sums_now[1:2], sums_now[2:3] + coarse_part
        if it == 0:
            curve = delta
        else:
            beta = gamma / gamma_old
            curve = delta + 2.0 * beta * cross + beta * beta * curve
        alpha = gamma / curve
        gamma_old = gamma

        total(0, hn.at[it], h_send.at[it], h_recv.at[it]).wait_recv()
        for f in range(6):
            plus = f % 2
            if plus:
                a = f // 2
                if it == 0:
                    new = u[f]
                else:
                    new = u[f] + beta * p[a]
                if not last:
                    p[a] = new
                if it == 0:
                    x_ref[a] = alpha * new
                else:
                    x_ref[a] = x_ref[a] + alpha * new
            elif last:
                continue
            rows = slice(32 * (f + 1), 32 * (f + 2))
            cols = jnp.concatenate([near_hi[0:32], near_hi[rows], near_lo[0:32], near_lo[rows]], axis=0)
            jump = loc[face * f:face * f + face, :] - hn[it, f].astype(F32) + dot(wide_t[f], cols)
            new = (signs[f] * masks[f]) * jump
            if it:
                new = new + beta * s[f]
            if last:
                res_ref[f // 2] = r[f] - alpha * new
            else:
                s[f] = new
                r[f] = r[f] - alpha * new
                precondition(f)

    for copy in sent:
        copy.wait_send()
    for it in range(ITERS):
        tall = sz.level if it == 0 else sz.block
        total(0, rxy.at[it, pl.ds(0, sz.lines - 1)], xy_send.at[it], xy_recv.at[it]).wait_send()
        total(0, sx.at[it, pl.ds(0, sz.chips - 1)], sx_send.at[it], sx_recv.at[it]).wait_send()
        total(0, sy.at[it, pl.ds(0, nz - 1)], sy_send.at[it], sy_recv.at[it]).wait_send()
        total(0, sp.at[it], sp_send.at[it], sp_recv.at[it]).wait_send()
        total(0, lev.at[it, 0, pl.ds(0, nz - 1), pl.ds(0, tall)], z_send.at[it], z_recv.at[it]).wait_send()
        total(0, lev.at[it, 0, pl.ds(0, nz), pl.ds(0, tall)], pp_send.at[it], pp_recv.at[it]).wait_send()
        total(0, hn.at[it], h_send.at[it], h_recv.at[it]).wait_send()


def body(sz, dual_rhs, local_flex, corner_coupling, face_stiffness, coarse_inverse, corner_ids):
    nx, ny, nz = sz.grid
    face, dofs, cases = sz.face, sz.dofs, sz.cases
    vmem, dma = pltpu.VMEM, pltpu.SemaphoreType.DMA
    g_rows = 7 * 32
    it = ITERS
    scratch = [
        vmem((3, face, cases), F32), vmem((dofs, dofs), BF16), vmem((24, dofs), BF16),
        vmem((6, face, face), BF16), vmem((sz.coarse, sz.coarse), BF16),
        vmem((sz.level, sz.lines * 16), BF16), vmem((32, 24), BF16),
        vmem((3, face, cases), BF16), vmem((3, face, cases), BF16), vmem((6, face, face), BF16),
        vmem((32, sz.wide), BF16), vmem((6, 32, sz.window), BF16), vmem((sz.wide, 128), F32),
        vmem((sz.window, 128), F32), vmem((6, face, 128), BF16), vmem((6, face, face), BF16),
        vmem((6, face, cases), F32), vmem((6, face, cases), F32), vmem((6, face, cases), F32),
        vmem((3, face, cases), F32), vmem((dofs, cases), F32), vmem((sz.wide, cases), BF16),
        vmem((dofs, cases), F32), vmem((it, 2, 16, cases), BF16), vmem((it, sz.lines, 16, cases), BF16),
        vmem((it, 2, nz, sz.level, cases), BF16), vmem((it, 6, face, cases), BF16),
        vmem((it, 6, face, cases), BF16), vmem((sz.rows, cases), BF16),
        vmem((sz.rows + g_rows, sz.rows), BF16), vmem((sz.rows, sz.coarse), BF16),
        vmem((sz.rows, sz.coarse), BF16),
        vmem((it, 3, 8, cases), F32), vmem((it, sz.chips, 8, cases), F32),
        vmem((it, nz, 8, cases), F32), vmem((it, 8, cases), F32),
        dma((7,)), dma((15,)), dma((6,)), dma((3,)), dma((6,)),
    ] + [dma((it,)) for _ in range(14)]
    anywhere = pl.BlockSpec(memory_space=pl.ANY)
    whole = pl.BlockSpec(memory_space=pltpu.VMEM)
    out = jax.ShapeDtypeStruct((3, face, cases), F32)
    x, res = pl.pallas_call(
        functools.partial(kernel, sz),
        out_shape=(out, out),
        in_specs=[pl.BlockSpec(memory_space=pltpu.SMEM)] + [anywhere] * 7,
        out_specs=(whole, whole),
        scratch_shapes=scratch,
        compiler_params=pltpu.CompilerParams(
            collective_id=0, has_side_effects=True, vmem_limit_bytes=56 * 1024 * 1024
        ),
        name="dual_cg",
    )(
        corner_ids.reshape(8), dual_rhs.reshape(3, face, cases), local_flex.reshape(dofs, dofs),
        corner_coupling.reshape(24, dofs), face_stiffness.reshape(6, face, face), coarse_inverse,
        jnp.asarray(plane_sums(sz), BF16), jnp.asarray(corner_order(), BF16),
    )
    return x[None, None, None], res[None, None, None]


def solution(mesh):
    grid = (mesh.shape["gx"], mesh.shape["gy"], mesh.shape["gz"])

    def run(dual_rhs, local_flex, corner_coupling, face_stiffness, coarse_inverse, corner_ids):
        sz = Sizes(grid, dual_rhs.shape[4], dual_rhs.shape[5], coarse_inverse.shape[0])
        deep = P("gx", "gy", "gz", None, None, None)
        mid = P("gx", "gy", "gz", None, None)
        return jax.shard_map(
            functools.partial(body, sz),
            mesh=mesh,
            in_specs=(deep, mid, mid, deep, P(), P("gx", "gy", "gz", None)),
            out_specs=(deep, deep),
            check_vma=False,
        )(dual_rhs, local_flex, corner_coupling, face_stiffness, coarse_inverse, corner_ids)

    return run
```

```python
import functools

import jax
import jax.numpy as jnp
import numpy as np
from jax import lax
from jax.experimental import pallas as pl
from jax.experimental.pallas import tpu as pltpu
from jax.sharding import PartitionSpec as P

ITERS = 3
MESH = pl.DeviceIdType.MESH
F32 = jnp.float32
BF16 = jnp.bfloat16


def up_to(value, step):
    return -(-value // step) * step


def iota(shape, dim):
    return lax.broadcasted_iota(jnp.int32, shape, dim)


def dot(left, right, contract=None):
    if contract is None:
        contract = (left.ndim - 1, 0)
    dims = (((contract[0],), (contract[1],)), ((), ()))
    return lax.dot_general(left, right, dims, preferred_element_type=F32)


class Sizes:
    def __init__(self, grid, face, cases, coarse):
        self.grid, self.face, self.cases, self.coarse = grid, face, cases, coarse
        self.dofs = 6 * face
        self.window = up_to(face + 127, 128)
        self.wide = max(up_to(self.dofs, 128), face * 5 // 128 * 128 + self.window)
        self.split = face // 128 * 128
        self.rest = face - self.split
        self.tall = up_to(face, 16)
        nx, ny, nz = grid
        self.plane = (nx - 1) * (ny - 1)
        self.block = up_to(3 * self.plane + 1, 16)
        self.names = up_to(self.plane, 16)
        self.rows = up_to(self.block * (nz - 1), 128)
        self.lines = nx * ny


def plane_sums(sz):
    nx, ny, _ = sz.grid
    table = np.zeros((sz.block + sz.names, sz.lines * 16), np.float32)
    for i in range(nx):
        for j in range(ny):
            first = (i * ny + j) * 16
            for kx in range(2):
                for ky in range(2):
                    x, y = i + kx, j + ky
                    if not (1 <= x < nx and 1 <= y < ny):
                        continue
                    spot = (x - 1) * (ny - 1) + y - 1
                    for d in range(3):
                        table[d * sz.plane + spot, first + (kx * 2 + ky) * 3 + d] = 1
            if i + 1 < nx and j + 1 < ny:
                table[sz.block + i * (ny - 1) + j, first] = 1
    return table


def corner_order():
    table = np.zeros((32, 24), np.float32)
    for kx in range(2):
        for ky in range(2):
            for kz in range(2):
                for d in range(3):
                    row = kz * 16 + (kx * 2 + ky) * 3 + d
                    table[row, 3 * (4 * kx + 2 * ky + kz) + d] = 1
    return table


def kernel(sz, ids, rhs_h, flex_h, coup_h, stiff_h, inv_h, sums_h, order_h,
           x_h, res_h,
           rhs, flex, coup, stiff, inv, sums, order,
           rhs_b, rhs_n, t_b, t_n, kn, kc, kc_n, cs, cf, cn, own_t, nb_t, ksum, wg,
           r, s, t, u, p, x, sg, sgb, loc, wl, ml, cpb, rxy, lev, hb, hn, bmat, ae, pm, pa,
           idb, idr, idz, ss, sx, sy,
           load_sem, i_send, k_recv, kc_recv, r_recv, t_recv, c_recv,
           id_send, id_recv, idz_send, idz_recv, out_sem,
           xy_send, xy_recv, z_send, z_recv, pp_send, pp_recv, h_send, h_recv,
           sx_send, sx_recv, sy_send, sy_recv):
    nx, ny, nz = sz.grid
    face, dofs, split, rest, tall = sz.face, sz.dofs, sz.split, sz.rest, sz.tall
    i, j, l = lax.axis_index("gx"), lax.axis_index("gy"), lax.axis_index("gz")
    core = lax.rem(i, 2)
    place = (i, j, l)
    partner = {"gx": i + 1 - 2 * core, "gy": j, "gz": l}

    def toward(f):
        axis, step = f // 2, f % 2
        size = sz.grid[axis]
        spot = list(place)
        spot[axis] = lax.rem(spot[axis] + (1 if step else size - 1), size)
        return dict(zip(("gx", "gy", "gz"), spot))

    spread = sorted(
        [(di, dj) for di in range(nx) for dj in range(ny) if di or dj],
        key=lambda o: -(min(o[0], nx - o[0]) / 2 + min(o[1], ny - o[1])),
    )
    lanes = sorted(range(1, nz), key=lambda o: -min(o, nz - o))

    def across(di, dj):
        return {"gx": lax.rem(i + di, nx), "gy": lax.rem(j + dj, ny), "gz": l}

    def along(dl):
        return {"gx": i, "gy": j, "gz": lax.rem(l + dl, nz)}

    def remote(src, dst, send, recv, target):
        return pltpu.make_async_remote_copy(
            src_ref=src, dst_ref=dst, send_sem=send, recv_sem=recv,
            device_id=target, device_id_type=MESH,
        )

    def total(piece, send_sem, recv_sem):
        return remote(piece, piece, send_sem, recv_sem, partner)

    def send(src, dst, send_sem, recv_sem, target):
        copy = remote(src, dst, send_sem, recv_sem, target)
        copy.start()
        return copy

    loads = {}

    def load(name, src, dst):
        copy = pltpu.make_async_copy(src, dst, load_sem.at[len(loads)])
        copy.start()
        loads[name] = copy

    for a in range(3):
        load(("rhs", a), rhs_h.at[pl.ds(face * a, face), 0], rhs.at[a])
    for f in (1, 3, 5, 0, 2, 4):
        load(("stiff", f), stiff_h.at[f], stiff.at[f])
    load("coup", coup_h, coup)
    load("order", order_h, order)
    load("sums", sums_h, sums)
    load("flex", flex_h, flex)
    load("inv", inv_h, inv)

    barrier = pltpu.get_barrier_semaphore()
    for di, dj in spread:
        pl.semaphore_signal(barrier, inc=1, device_id=across(di, dj), device_id_type=MESH)
    for dl in lanes:
        pl.semaphore_signal(barrier, inc=1, device_id=along(dl), device_id_type=MESH)

    masks = []
    for f in range(6):
        axis, step = f // 2, f % 2
        edge = place[axis] < sz.grid[axis] - 1 if step else place[axis] > 0
        masks.append(jnp.where(edge, 1.0, 0.0).astype(F32))
    signs = [-1.0, 1.0] * 3

    for a in range(3):
        loads["rhs", a].wait()
        rhs_b[a] = rhs[a].astype(BF16)
        r[a] = rhs[a] * masks[2 * a + 1]
    for a in range(3):
        loads["stiff", 2 * a + 1].wait()
        t_b[a] = dot(stiff[2 * a + 1], rhs_b[a]).astype(BF16)
    kc[...] = jnp.zeros_like(kc)
    for f in (0, 2, 4, 1, 3, 5):
        if f % 2 == 0:
            loads["stiff", f].wait()
        kc[f, :, 0:rest] = stiff[f, split:face, split:face]
    idb[...] = jnp.full((16, sz.cases), ids[7], jnp.int32).astype(F32).astype(BF16)

    pl.semaphore_wait(barrier, len(spread) + len(lanes))

    sent = []

    def send_stiff(f):
        g = f ^ 1
        sent.append(send(stiff.at[f, :, pl.ds(0, split)], kn.at[g], i_send.at[f], k_recv.at[g], toward(f)))
        sent.append(send(kc.at[f], kc_n.at[g], i_send.at[6 + f], kc_recv.at[g], toward(f)))

    for a in range(3):
        sent.append(send(rhs_b.at[a], rhs_n.at[a], i_send.at[12 + a], r_recv.at[a], toward(2 * a + 1)))
        send_stiff(2 * a)
    for a in range(3):
        sent.append(send(t_b.at[a], t_n.at[a], i_send.at[15 + a], t_recv.at[a], toward(2 * a + 1)))
    slot = i * ny + j
    for di, dj in spread:
        send(idb, idr.at[slot], id_send, id_recv, across(di, dj))
    idr[slot] = idb[...]

    loads["coup"].wait()
    loads["order"].wait()
    cs[...] = jnp.zeros_like(cs)
    cs[:, 0:dofs] = dot(order[...], coup[...]).astype(BF16)
    starts = [face * f // 128 * 128 for f in range(6)]
    for f in range(6):
        off = face * f - starts[f]
        near = cs[:, starts[f]:starts[f] + sz.window].astype(F32)
        cf[f] = (signs[f] * near[:, off:off + face]).astype(BF16)
    pick_row, pick_col = iota((32, 128), 0), iota((32, 128), 1)
    pick_own = ((pick_col & 63) == pick_row).astype(F32).astype(BF16)
    pick_nb = -((pick_col & 63) == pick_row + 32).astype(F32).astype(BF16)
    own_t[...] = dot(cs[...], pick_own, (0, 0))

    g_rows = 7 * 32
    line = iota((g_rows, 128), 0)
    g, kz, e = line >> 5, (line >> 4) & 1, line & 15
    third = (e * 11) >> 5
    d, kx, ky = e - 3 * third, third >> 1, third & 1

    def shift(minus, plus):
        return (g == plus).astype(jnp.int32) - (g == minus).astype(jnp.int32)

    gx = i + kx + shift(1, 2)
    gy = j + ky + shift(3, 4)
    gz = l + kz + shift(5, 6)
    inside = (e < 12) & (gx >= 1) & (gx < nx) & (gy >= 1) & (gy < ny) & (gz >= 1) & (gz < nz)
    spot = jnp.where(
        inside, sz.block * (gz - 1) + sz.plane * d + (ny - 1) * (gx - 1) + gy - 1, -1
    )
    for k in range(sz.rows // 128):
        ae[sz.rows:sz.rows + g_rows, 128 * k:128 * k + 128] = (
            (iota((g_rows, 128), 1) + 128 * k == spot).astype(F32).astype(BF16)
        )
    bmat[...] = jnp.zeros_like(bmat)
    pm[...] = jnp.zeros_like(pm)
    wg[...] = jnp.zeros_like(wg)
    eye = (iota((rest, 128), 0) == iota((rest, 128), 1)).astype(F32).astype(BF16)

    def add_stiffness(f):
        for copy in (
            remote(kn.at[f], kn.at[f], i_send.at[f], k_recv.at[f], toward(f)),
            remote(kc.at[f], kc_n.at[f], i_send.at[6 + f], kc_recv.at[f], toward(f)),
        ):
            copy.wait_recv()
        both = (stiff[f, :, 0:split].astype(F32) + kn[f].astype(F32)).astype(BF16)
        ksum[f, :, 0:split] = both
        turned = dot(both[split:face], eye, (0, 0))
        ksum[f, 0:split, split:face] = turned[:, 0:rest].astype(BF16)
        ksum[f, split:face, split:face] = (
            stiff[f, split:face, split:face].astype(F32) + kc_n[f, :, 0:rest].astype(F32)
        ).astype(BF16)

    for a in range(3):
        remote(rhs_b.at[a], rhs_n.at[a], i_send.at[12 + a], r_recv.at[a], partner).wait_recv()
        part = dot(stiff[2 * a], rhs_n[a])
        add_stiffness(2 * a + 1)
        u[0, 2 * a + 1] = (0.25 * masks[2 * a + 1]) * dot(ksum[2 * a + 1], rhs_b[a])
        remote(t_b.at[a], t_n.at[a], i_send.at[15 + a], t_recv.at[a], partner).wait_recv()
        u[0, 2 * a] = (0.25 * masks[2 * a]) * (part + t_n[a].astype(F32))

    alpha = beta = gamma_old = curve = None
    for it in range(ITERS):
        last = it + 1 == ITERS
        now, then = it % 2, (it + 1) % 2
        cp = None
        for f in range(6):
            piece = dot(cf[f], u[now, f].astype(BF16))
            cp = piece if cp is None else cp + piece
        low, high = cp[0:16].astype(BF16), cp[16:32].astype(BF16)
        cpb[it, 0] = low
        cpb[it, 1] = high
        for di, dj in spread:
            target = across(di, dj)
            send(cpb.at[it, lax.rem(target["gx"], 2)], rxy.at[it, slot], xy_send.at[it],
                 xy_recv.at[it], target)
        rxy[it, slot] = jnp.where(core == 0, low.astype(F32), high.astype(F32)).astype(BF16)
        if it == 0:
            for f in (1, 3, 5):
                send_stiff(f)
            for f in range(6):
                sent.append(
                    send(cs.at[:, pl.ds(starts[f], sz.window)], cn.at[f ^ 1], i_send.at[18 + f],
                         c_recv.at[f ^ 1], toward(f))
                )
            total(idr.at[pl.ds(0, sz.lines - 1)], id_send, id_recv).wait_recv()
            loads["sums"].wait()
            idz[l] = dot(sums[sz.block:], idr[...].reshape(sz.lines * 16, sz.cases)).astype(BF16)
            for dl in lanes:
                send(idz.at[l], idz.at[l], idz_send, idz_recv, along(dl))

        for f in range(6):
            sg[face * f:face * f + face, :] = signs[f] * u[now, f]
        sgb[...] = sg[...].astype(BF16)
        if it == 0:
            loads["flex"].wait()
        loc[...] = dot(flex[...], sgb[...])
        delta = jnp.sum(sgb[...].astype(F32) * loc[...], axis=0, keepdims=True)
        for a in range(3):
            f = 2 * a + 1
            if it == 0:
                continue
            new = u[then, f]
            if it > 1:
                new = new + beta * p[a]
            p[a] = new
            x[a] = alpha * new if it == 1 else x[a] + alpha * new
            r[a] = r[a] - alpha * s[a]
        gamma = sum(jnp.sum(r[a] * u[now, 2 * a + 1], axis=0, keepdims=True) for a in range(3))
        if it:
            cross = sum(jnp.sum(s[a] * u[now, 2 * a + 1], axis=0, keepdims=True) for a in range(3))
        else:
            cross = jnp.zeros_like(gamma)
        where = iota((4, sz.cases), 0)
        packed = jnp.where(where == 0, gamma, jnp.where(where == 1, cross, jnp.where(where == 2, delta, 0.0)))
        ss[it, 0] = packed
        sx[it, slot] = packed
        for di, dj in spread:
            send(ss.at[it, 0], sx.at[it, slot], sx_send.at[it], sx_recv.at[it], across(di, dj))
        for f in range(6):
            hb[it, f] = loc[face * f:face * f + face, :].astype(BF16)
            send(hb.at[it, f], hn.at[it, f ^ 1], h_send.at[it], h_recv.at[it], toward(f))

        total(rxy.at[it, pl.ds(0, sz.lines - 1)], xy_send.at[it], xy_recv.at[it]).wait_recv()
        lev[it, core, l] = dot(sums[0:sz.block], rxy[it].reshape(sz.lines * 16, sz.cases)).astype(BF16)
        for dl in lanes:
            piece = lev.at[it, core, l]
            send(piece, piece, z_send.at[it], z_recv.at[it], along(dl))

        total(hn.at[it], h_send.at[it], h_recv.at[it]).wait_recv()

        def local_jump(f):
            jump = (signs[f] * masks[f]) * (loc[face * f:face * f + face, :] - hn[it, f].astype(F32))
            if f % 2:
                wl[f // 2] = jump
            if not last:
                ml[f] = (0.25 * masks[f]) * dot(ksum[f], jump.astype(BF16))

        for f in (1, 3, 5) if it == 0 or last else range(6):
            local_jump(f)

        total(sx.at[it, pl.ds(0, sz.lines - 1)], sx_send.at[it], sx_recv.at[it]).wait_recv()
        packed = jnp.sum(sx[it], axis=0)
        ss[it, 1] = packed
        sy[it, l] = packed
        for dl in lanes:
            send(ss.at[it, 1], sy.at[it, l], sy_send.at[it], sy_recv.at[it], along(dl))

        if it == 0:
            for f in (0, 2, 4):
                add_stiffness(f)
                local_jump(f)
            for f in range(6):
                remote(cs.at[:, pl.ds(starts[f], sz.window)], cn.at[f], i_send.at[18 + f],
                       c_recv.at[f], toward(f)).wait_recv()
                nb_t[...] = dot(cn[f], pick_nb, (0, 0))
                off = face * (f ^ 1) - starts[f ^ 1]
                wide = (signs[f] * masks[f]) * (own_t[face * f:face * f + face, :] + nb_t[off:off + face, :])
                wide = wide.astype(BF16)
                wg[f, 0:face, :] = wide
                wg[f, tall:tall + face, :] = ((0.25 * masks[f]) * dot(ksum[f], wide)).astype(BF16)

            small_r, small_c = iota((sz.block, sz.names), 0), iota((sz.block, sz.names), 1)
            part = (small_r >= sz.plane).astype(jnp.int32) + (small_r >= 2 * sz.plane).astype(jnp.int32)
            expand = ((small_c == small_r - sz.plane * part) & (small_r < 3 * sz.plane)).astype(F32).astype(BF16)
            rr = iota((sz.block, 128), 0)
            comp = (rr >= sz.plane).astype(jnp.int32) + (rr >= 2 * sz.plane).astype(jnp.int32)
            total(idz.at[pl.ds(0, nz - 1)], idz_send, idz_recv).wait_recv()
            for z in range(1, nz):
                here = pl.ds(sz.block * (z - 1), sz.block)
                col = 3.0 * dot(expand, idz[z - 1]) + comp.astype(F32)
                col = jnp.where(rr < 3 * sz.plane, col, -1.0)
                for k in range(up_to(sz.coarse, 128) // 128):
                    width = min(128, sz.coarse - 128 * k)
                    at = (iota((sz.block, 128), 1) + 128 * k).astype(F32)
                    pm[here, 128 * k:128 * k + width] = (at == col).astype(F32).astype(BF16)[:, 0:width]
            loads["inv"].wait()
            pa[...] = dot(pm[...], inv[...]).astype(BF16)
            ae[0:sz.rows, :] = dot(pa[...], pm[...], (1, 1)).astype(BF16)
            ae[sz.rows:sz.rows + g_rows, :] = dot(ae[sz.rows:sz.rows + g_rows, :], ae[0:sz.rows, :]).astype(BF16)

        total(lev.at[it, 0, pl.ds(0, nz - 1)], z_send.at[it], z_recv.at[it]).wait_recv()
        piece = lev.at[it, core]
        send(piece, piece, pp_send.at[it], pp_recv.at[it], partner)
        total(piece, pp_send.at[it], pp_recv.at[it]).wait_recv()

        for z in range(1, nz):
            level = lev[it, 0, z].astype(F32) + lev[it, 1, z - 1].astype(F32)
            bmat[sz.block * (z - 1):sz.block * z, :] = level.astype(BF16)
        sol = dot(ae[...], bmat[...])
        coarse_part = jnp.sum(sol[0:sz.rows] * bmat[...].astype(F32), axis=0, keepdims=True)
        near = sol[sz.rows:]
        near_hi = near.astype(BF16)
        near_lo = (near - near_hi.astype(F32)).astype(BF16)

        total(sy.at[it, pl.ds(0, nz - 1)], sy_send.at[it], sy_recv.at[it]).wait_recv()
        sums_now = jnp.sum(sy[it], axis=0)
        gamma, cross, delta = sums_now[0:1], sums_now[1:2], sums_now[2:3] + coarse_part
        if it == 0:
            curve = delta
        else:
            beta = gamma / gamma_old
            curve = delta + 2.0 * beta * cross + beta * beta * curve
        alpha = gamma / curve
        gamma_old = gamma

        for f in (1, 3, 5) if last else range(6):
            rows = slice(32 * (f + 1), 32 * (f + 2))
            cols = jnp.concatenate([near_hi[0:32], near_hi[rows], near_lo[0:32], near_lo[rows]], axis=0)
            a = f // 2
            if last:
                new = wl[a] + dot(wg[f, 0:face, :], cols) + beta * s[a]
                res = r[a] - alpha * new
                sum_p = u[now, f] + beta * p[a]
                r[a] = res
                x[a] = x[a] + alpha * sum_p
                continue
            both = dot(wg[f], cols)
            turned = ml[f] + both[tall:tall + face]
            if it:
                turned = turned + beta * t[f]
            t[f] = turned
            u[then, f] = u[now, f] - alpha * turned
            if f % 2:
                new = wl[a] + both[0:face]
                s[a] = new if it == 0 else new + beta * s[a]

    outs = []
    for a in range(3):
        for n, (src, dst) in enumerate(((x, x_h), (r, res_h))):
            copy = pltpu.make_async_copy(src.at[a], dst.at[pl.ds(face * a, face), 0], out_sem.at[n, a])
            copy.start()
            outs.append(copy)
    for copy in sent:
        copy.wait_send()
    total(idr.at[pl.ds(0, sz.lines - 1)], id_send, id_recv).wait_send()
    total(idz.at[pl.ds(0, nz - 1)], idz_send, idz_recv).wait_send()
    for it in range(ITERS):
        total(rxy.at[it, pl.ds(0, sz.lines - 1)], xy_send.at[it], xy_recv.at[it]).wait_send()
        total(sx.at[it, pl.ds(0, sz.lines - 1)], sx_send.at[it], sx_recv.at[it]).wait_send()
        total(sy.at[it, pl.ds(0, nz - 1)], sy_send.at[it], sy_recv.at[it]).wait_send()
        total(lev.at[it, 0, pl.ds(0, nz - 1)], z_send.at[it], z_recv.at[it]).wait_send()
        total(lev.at[it, 0], pp_send.at[it], pp_recv.at[it]).wait_send()
        total(hn.at[it], h_send.at[it], h_recv.at[it]).wait_send()
    for copy in outs:
        copy.wait()


def body(sz, dual_rhs, local_flex, corner_coupling, face_stiffness, coarse_inverse, corner_ids):
    nx, ny, nz = sz.grid
    face, dofs, cases = sz.face, sz.dofs, sz.cases
    vmem, dma = pltpu.VMEM, pltpu.SemaphoreType.DMA
    g_rows = 7 * 32
    it = ITERS
    scratch = [
        vmem((3, face, cases), F32), vmem((dofs, dofs), BF16), vmem((24, dofs), BF16),
        vmem((6, face, face), BF16), vmem((sz.coarse, sz.coarse), BF16),
        vmem((sz.block + sz.names, sz.lines * 16), BF16), vmem((32, 24), BF16),
        vmem((3, face, cases), BF16), vmem((3, face, cases), BF16),
        vmem((3, face, cases), BF16), vmem((3, face, cases), BF16),
        vmem((6, face, sz.split), BF16), vmem((6, sz.rest, 128), BF16), vmem((6, sz.rest, 128), BF16),
        vmem((32, sz.wide), BF16), vmem((6, 32, face), BF16), vmem((6, 32, sz.window), BF16),
        vmem((sz.wide, 128), F32), vmem((sz.window, 128), F32), vmem((6, face, face), BF16),
        vmem((6, 2 * sz.tall, 128), BF16),
        vmem((3, face, cases), F32), vmem((3, face, cases), F32), vmem((6, face, cases), F32),
        vmem((2, 6, face, cases), F32), vmem((3, face, cases), F32), vmem((3, face, cases), F32),
        vmem((dofs, cases), F32), vmem((dofs, cases), BF16), vmem((dofs, cases), F32),
        vmem((3, face, cases), F32), vmem((6, face, cases), F32),
        vmem((it, 2, 16, cases), BF16), vmem((it, sz.lines, 16, cases), BF16),
        vmem((it, 2, nz, sz.block, cases), BF16), vmem((it, 6, face, cases), BF16),
        vmem((it, 6, face, cases), BF16), vmem((sz.rows, cases), BF16),
        vmem((sz.rows + g_rows, sz.rows), BF16), vmem((sz.rows, sz.coarse), BF16),
        vmem((sz.rows, sz.coarse), BF16),
        vmem((16, cases), BF16), vmem((sz.lines, 16, cases), BF16), vmem((nz, sz.names, cases), BF16),
        vmem((it, 2, 4, cases), F32), vmem((it, sz.lines, 4, cases), F32), vmem((it, nz, 4, cases), F32),
        dma((14,)), dma((24,)), dma((6,)), dma((6,)), dma((3,)), dma((3,)), dma((6,)),
        dma, dma, dma, dma, dma((2, 3)),
    ] + [dma((it,)) for _ in range(12)]
    anywhere = pl.BlockSpec(memory_space=pl.ANY)
    out = jax.ShapeDtypeStruct((3 * face, 1, cases), F32)
    x, res = pl.pallas_call(
        functools.partial(kernel, sz),
        out_shape=(out, out),
        in_specs=[pl.BlockSpec(memory_space=pltpu.SMEM)] + [anywhere] * 7,
        out_specs=(anywhere, anywhere),
        scratch_shapes=scratch,
        compiler_params=pltpu.CompilerParams(
            collective_id=0, has_side_effects=True, vmem_limit_bytes=56 * 1024 * 1024
        ),
        name="dual_cg",
    )(
        corner_ids.reshape(8), dual_rhs.reshape(3 * face, 1, cases), local_flex.reshape(dofs, dofs),
        corner_coupling.reshape(24, dofs), face_stiffness.reshape(6, face, face), coarse_inverse,
        jnp.asarray(plane_sums(sz), BF16), jnp.asarray(corner_order(), BF16),
    )
    shape = (1, 1, 1, 3, face, cases)
    return x.reshape(shape), res.reshape(shape)


def solution(mesh):
    grid = (mesh.shape["gx"], mesh.shape["gy"], mesh.shape["gz"])

    def run(dual_rhs, local_flex, corner_coupling, face_stiffness, coarse_inverse, corner_ids):
        sz = Sizes(grid, dual_rhs.shape[4], dual_rhs.shape[5], coarse_inverse.shape[0])
        deep = P("gx", "gy", "gz", None, None, None)
        mid = P("gx", "gy", "gz", None, None)
        return jax.shard_map(
            functools.partial(body, sz),
            mesh=mesh,
            in_specs=(deep, mid, mid, deep, P(), P("gx", "gy", "gz", None)),
            out_specs=(deep, deep),
            check_vma=False,
        )(dual_rhs, local_flex, corner_coupling, face_stiffness, coarse_inverse, corner_ids)

    return run
```

```python
import functools

import jax
import jax.numpy as jnp
import numpy as np
from jax import lax
from jax.experimental import pallas as pl
from jax.experimental.pallas import tpu as pltpu
from jax.sharding import PartitionSpec as P

ITERS = 3
MESH = pl.DeviceIdType.MESH
F32 = jnp.float32
BF16 = jnp.bfloat16


def up_to(value, step):
    return -(-value // step) * step


def iota(shape, dim):
    return lax.broadcasted_iota(jnp.int32, shape, dim)


def dot(left, right, contract=None):
    if contract is None:
        contract = (left.ndim - 1, 0)
    dims = (((contract[0],), (contract[1],)), ((), ()))
    return lax.dot_general(left, right, dims, preferred_element_type=F32)


class Sizes:
    def __init__(self, grid, face, cases, coarse):
        self.grid, self.face, self.cases, self.coarse = grid, face, cases, coarse
        self.dofs = 6 * face
        self.window = up_to(face + 127, 128)
        self.wide = max(up_to(self.dofs, 128), face * 5 // 128 * 128 + self.window)
        self.split = face // 128 * 128
        self.rest = face - self.split
        self.tall = up_to(face, 16)
        nx, ny, nz = grid
        self.plane = (nx - 1) * (ny - 1)
        self.block = up_to(3 * self.plane + 1, 16)
        self.names = up_to(self.plane, 16)
        self.rows = up_to(self.block * (nz - 1), 128)
        self.lines = nx * ny


def plane_sums(sz):
    nx, ny, _ = sz.grid
    table = np.zeros((sz.block, sz.lines * 16), np.float32)
    names = np.zeros((sz.names, sz.lines * 8), np.float32)
    for i in range(nx):
        for j in range(ny):
            first = (i * ny + j) * 16
            for kx in range(2):
                for ky in range(2):
                    x, y = i + kx, j + ky
                    if not (1 <= x < nx and 1 <= y < ny):
                        continue
                    spot = (x - 1) * (ny - 1) + y - 1
                    for d in range(3):
                        table[d * sz.plane + spot, first + (kx * 2 + ky) * 3 + d] = 1
            if i + 1 < nx and j + 1 < ny:
                names[i * (ny - 1) + j, first // 2] = 1
    return table, names


def corner_order():
    table = np.zeros((32, 24), np.float32)
    for kx in range(2):
        for ky in range(2):
            for kz in range(2):
                for d in range(3):
                    row = kz * 16 + (kx * 2 + ky) * 3 + d
                    table[row, 3 * (4 * kx + 2 * ky + kz) + d] = 1
    return table


def kernel(sz, ids_h, rhs_h, flex_h, coup_h, stiff_h, inv_h, sums_h, sums_n_h, order_h,
           x, r,
           ids, rhs, flex, coup, stiff, inv, sums, sums_n, order,
           rhs_b, rhs_n, t_b, t_n, kn, kc, kc_n, cs, cf, cn, own_t, nb_t, ksum, wg,
           s, t, u, p, sg, sgb, loc, wl, ml, cpb, rxy, lev, hb, hn, bmat, ae, pm, pa,
           idb, idr, idz, ss, sx, sy,
           load_sem, i_send, k_recv, kc_recv, r_recv, t_recv, c_recv,
           id_send, id_recv, idz_send, idz_recv,
           xy_send, xy_recv, z_send, z_recv, pp_send, pp_recv, h_send, h_recv,
           sx_send, sx_recv, sy_send, sy_recv):
    nx, ny, nz = sz.grid
    face, dofs, split, rest, tall = sz.face, sz.dofs, sz.split, sz.rest, sz.tall
    i, j, l = lax.axis_index("gx"), lax.axis_index("gy"), lax.axis_index("gz")
    core = lax.rem(i, 2)
    place = (i, j, l)
    partner = {"gx": i + 1 - 2 * core, "gy": j, "gz": l}

    def toward(f):
        axis, step = f // 2, f % 2
        size = sz.grid[axis]
        spot = list(place)
        spot[axis] = lax.rem(spot[axis] + (1 if step else size - 1), size)
        return dict(zip(("gx", "gy", "gz"), spot))

    spread = sorted(
        [(di, dj) for di in range(nx) for dj in range(ny) if di or dj],
        key=lambda o: -(min(o[0], nx - o[0]) / 2 + min(o[1], ny - o[1])),
    )
    lanes = sorted(range(1, nz), key=lambda o: -min(o, nz - o))

    def across(di, dj):
        return {"gx": lax.rem(i + di, nx), "gy": lax.rem(j + dj, ny), "gz": l}

    def along(dl):
        return {"gx": i, "gy": j, "gz": lax.rem(l + dl, nz)}

    def remote(src, dst, send, recv, target):
        return pltpu.make_async_remote_copy(
            src_ref=src, dst_ref=dst, send_sem=send, recv_sem=recv,
            device_id=target, device_id_type=MESH,
        )

    def total(piece, send_sem, recv_sem):
        return remote(piece, piece, send_sem, recv_sem, partner)

    def send(src, dst, send_sem, recv_sem, target):
        copy = remote(src, dst, send_sem, recv_sem, target)
        copy.start()
        return copy

    loads = {}

    def load(name, src, dst):
        copy = pltpu.make_async_copy(src, dst, load_sem.at[len(loads)])
        copy.start()
        loads[name] = copy

    load("ids", ids_h, ids)
    for a in range(3):
        load(("rhs", a), rhs_h.at[pl.ds(face * a, face), 0], rhs.at[a])
    for f in (1, 3, 5, 0, 2, 4):
        load(("stiff", f), stiff_h.at[f], stiff.at[f])
    load("coup", coup_h, coup)
    load("order", order_h, order)
    load("sums", sums_h, sums)
    load("sums_n", sums_n_h, sums_n)
    load("flex", flex_h, flex)
    load("inv", inv_h, inv)

    barrier = pltpu.get_barrier_semaphore()
    for di, dj in spread:
        pl.semaphore_signal(barrier, inc=1, device_id=across(di, dj), device_id_type=MESH)
    for dl in lanes:
        pl.semaphore_signal(barrier, inc=1, device_id=along(dl), device_id_type=MESH)

    masks = []
    for f in range(6):
        axis, step = f // 2, f % 2
        edge = place[axis] < sz.grid[axis] - 1 if step else place[axis] > 0
        masks.append(jnp.where(edge, 1.0, 0.0).astype(F32))
    signs = [-1.0, 1.0] * 3

    for a in range(3):
        loads["rhs", a].wait()
        rhs_b[a] = rhs[a].astype(BF16)
        r[a] = rhs[a] * masks[2 * a + 1]
    for a in range(3):
        loads["stiff", 2 * a + 1].wait()
        t_b[a] = dot(stiff[2 * a + 1], rhs_b[a]).astype(BF16)
    kc[...] = jnp.zeros_like(kc)
    for f in (0, 2, 4, 1, 3, 5):
        if f % 2 == 0:
            loads["stiff", f].wait()
        kc[f, :, 0:rest] = stiff[f, split:face, split:face]
    loads["ids"].wait()
    idb[...] = jnp.full((8, sz.cases), ids[7], jnp.int32).astype(F32).astype(BF16)

    pl.semaphore_wait(barrier, len(spread) + len(lanes))

    sent = []

    def send_stiff(f):
        g = f ^ 1
        sent.append(send(stiff.at[f, :, pl.ds(0, split)], kn.at[g], i_send.at[f], k_recv.at[g], toward(f)))
        sent.append(send(kc.at[f], kc_n.at[g], i_send.at[6 + f], kc_recv.at[g], toward(f)))

    for a in range(3):
        sent.append(send(rhs_b.at[a], rhs_n.at[a], i_send.at[12 + a], r_recv.at[a], toward(2 * a + 1)))
        send_stiff(2 * a)
    for a in range(3):
        sent.append(send(t_b.at[a], t_n.at[a], i_send.at[15 + a], t_recv.at[a], toward(2 * a + 1)))
    slot = i * ny + j
    for di, dj in spread:
        send(idb, idr.at[slot], id_send, id_recv, across(di, dj))
    idr[slot] = idb[...]

    loads["coup"].wait()
    loads["order"].wait()
    cs[...] = jnp.zeros_like(cs)
    cs[:, 0:dofs] = dot(order[...], coup[...]).astype(BF16)
    starts = [face * f // 128 * 128 for f in range(6)]
    for f in range(6):
        sent.append(
            send(cs.at[:, pl.ds(starts[f], sz.window)], cn.at[f ^ 1], i_send.at[18 + f],
                 c_recv.at[f ^ 1], toward(f))
        )
    for f in (1, 3, 5):
        send_stiff(f)
    for f in range(6):
        off = face * f - starts[f]
        near = cs[:, starts[f]:starts[f] + sz.window].astype(F32)
        cf[f] = (signs[f] * near[:, off:off + face]).astype(BF16)
    pick_row, pick_col = iota((32, 128), 0), iota((32, 128), 1)
    pick_own = ((pick_col & 63) == pick_row).astype(F32).astype(BF16)
    pick_nb = -((pick_col & 63) == pick_row + 32).astype(F32).astype(BF16)
    own_t[...] = dot(cs[...], pick_own, (0, 0))

    g_rows = 7 * 32
    line = iota((g_rows, 128), 0)
    g, kz, e = line >> 5, (line >> 4) & 1, line & 15
    third = (e * 11) >> 5
    d, kx, ky = e - 3 * third, third >> 1, third & 1

    def shift(minus, plus):
        return (g == plus).astype(jnp.int32) - (g == minus).astype(jnp.int32)

    gx = i + kx + shift(1, 2)
    gy = j + ky + shift(3, 4)
    gz = l + kz + shift(5, 6)
    inside = (e < 12) & (gx >= 1) & (gx < nx) & (gy >= 1) & (gy < ny) & (gz >= 1) & (gz < nz)
    spot = jnp.where(
        inside, sz.block * (gz - 1) + sz.plane * d + (ny - 1) * (gx - 1) + gy - 1, -1
    )
    for k in range(sz.rows // 128):
        ae[sz.rows:sz.rows + g_rows, 128 * k:128 * k + 128] = (
            (iota((g_rows, 128), 1) + 128 * k == spot).astype(F32).astype(BF16)
        )
    bmat[...] = jnp.zeros_like(bmat)
    pm[...] = jnp.zeros_like(pm)
    wg[...] = jnp.zeros_like(wg)
    eye = (iota((rest, 128), 0) == iota((rest, 128), 1)).astype(F32).astype(BF16)

    def add_stiffness(f):
        for copy in (
            remote(kn.at[f], kn.at[f], i_send.at[f], k_recv.at[f], toward(f)),
            remote(kc.at[f], kc_n.at[f], i_send.at[6 + f], kc_recv.at[f], toward(f)),
        ):
            copy.wait_recv()
        both = (stiff[f, :, 0:split].astype(F32) + kn[f].astype(F32)).astype(BF16)
        ksum[f, :, 0:split] = both
        turned = dot(both[split:face], eye, (0, 0))
        ksum[f, 0:split, split:face] = turned[:, 0:rest].astype(BF16)
        ksum[f, split:face, split:face] = (
            stiff[f, split:face, split:face].astype(F32) + kc_n[f, :, 0:rest].astype(F32)
        ).astype(BF16)

    for a in range(3):
        remote(rhs_b.at[a], rhs_n.at[a], i_send.at[12 + a], r_recv.at[a], partner).wait_recv()
        part = dot(stiff[2 * a], rhs_n[a])
        add_stiffness(2 * a + 1)
        u[0, 2 * a + 1] = (0.25 * masks[2 * a + 1]) * dot(ksum[2 * a + 1], rhs_b[a])
        remote(t_b.at[a], t_n.at[a], i_send.at[15 + a], t_recv.at[a], partner).wait_recv()
        u[0, 2 * a] = (0.25 * masks[2 * a]) * (part + t_n[a].astype(F32))

    alpha = beta = gamma_old = curve = None
    for it in range(ITERS):
        last = it + 1 == ITERS
        now, then = it % 2, (it + 1) % 2
        cp = None
        for f in range(6):
            piece = dot(cf[f], u[now, f].astype(BF16))
            cp = piece if cp is None else cp + piece
        low, high = cp[0:16].astype(BF16), cp[16:32].astype(BF16)
        cpb[it, 0] = low
        cpb[it, 1] = high
        for di, dj in spread:
            target = across(di, dj)
            send(cpb.at[it, lax.rem(target["gx"], 2)], rxy.at[it, slot], xy_send.at[it],
                 xy_recv.at[it], target)
        rxy[it, slot] = jnp.where(core == 0, low.astype(F32), high.astype(F32)).astype(BF16)
        if it == 0:
            total(idr.at[pl.ds(0, sz.lines - 1)], id_send, id_recv).wait_recv()
            loads["sums"].wait()
            loads["sums_n"].wait()
            idz[l] = dot(sums_n[...], idr[...].reshape(sz.lines * 8, sz.cases)).astype(BF16)
            for dl in lanes:
                send(idz.at[l], idz.at[l], idz_send, idz_recv, along(dl))

        for f in range(6):
            sg[face * f:face * f + face, :] = signs[f] * u[now, f]
        sgb[...] = sg[...].astype(BF16)
        if it == 0:
            loads["flex"].wait()
        loc[...] = dot(flex[...], sgb[...])
        delta = jnp.sum(sgb[...].astype(F32) * loc[...], axis=0, keepdims=True)
        for a in range(3):
            f = 2 * a + 1
            if it == 0:
                continue
            new = u[then, f]
            if it > 1:
                new = new + beta * p[a]
            p[a] = new
            x[a] = alpha * new if it == 1 else x[a] + alpha * new
            r[a] = r[a] - alpha * s[a]
        gamma = sum(jnp.sum(r[a] * u[now, 2 * a + 1], axis=0, keepdims=True) for a in range(3))
        if it:
            cross = sum(jnp.sum(s[a] * u[now, 2 * a + 1], axis=0, keepdims=True) for a in range(3))
        else:
            cross = jnp.zeros_like(gamma)
        where = iota((4, sz.cases), 0)
        packed = jnp.where(where == 0, gamma, jnp.where(where == 1, cross, jnp.where(where == 2, delta, 0.0)))
        ss[it, 0] = packed
        sx[it, slot] = packed
        for di, dj in spread:
            send(ss.at[it, 0], sx.at[it, slot], sx_send.at[it], sx_recv.at[it], across(di, dj))
        for f in range(6):
            hb[it, f] = loc[face * f:face * f + face, :].astype(BF16)
            send(hb.at[it, f], hn.at[it, f ^ 1], h_send.at[it], h_recv.at[it], toward(f))

        if it == 0:
            for f in (0, 2, 4):
                add_stiffness(f)
            for f in range(6):
                remote(cs.at[:, pl.ds(starts[f], sz.window)], cn.at[f], i_send.at[18 + f],
                       c_recv.at[f], toward(f)).wait_recv()
                nb_t[...] = dot(cn[f], pick_nb, (0, 0))
                off = face * (f ^ 1) - starts[f ^ 1]
                wide = (signs[f] * masks[f]) * (own_t[face * f:face * f + face, :] + nb_t[off:off + face, :])
                wide = wide.astype(BF16)
                wg[f, 0:face, :] = wide
                wg[f, tall:tall + face, :] = ((0.25 * masks[f]) * dot(ksum[f], wide)).astype(BF16)

        total(rxy.at[it, pl.ds(0, sz.lines - 1)], xy_send.at[it], xy_recv.at[it]).wait_recv()
        lev[it, core, l] = dot(sums[...], rxy[it].reshape(sz.lines * 16, sz.cases)).astype(BF16)
        for dl in lanes:
            piece = lev.at[it, core, l]
            send(piece, piece, z_send.at[it], z_recv.at[it], along(dl))

        if it == 0:
            small_r, small_c = iota((sz.block, sz.names), 0), iota((sz.block, sz.names), 1)
            part = (small_r >= sz.plane).astype(jnp.int32) + (small_r >= 2 * sz.plane).astype(jnp.int32)
            expand = ((small_c == small_r - sz.plane * part) & (small_r < 3 * sz.plane)).astype(F32).astype(BF16)
            rr = iota((sz.block, 128), 0)
            comp = (rr >= sz.plane).astype(jnp.int32) + (rr >= 2 * sz.plane).astype(jnp.int32)
            total(idz.at[pl.ds(0, nz - 1)], idz_send, idz_recv).wait_recv()
            for z in range(1, nz):
                here = pl.ds(sz.block * (z - 1), sz.block)
                col = 3.0 * dot(expand, idz[z - 1]) + comp.astype(F32)
                col = jnp.where(rr < 3 * sz.plane, col, -1.0)
                for k in range(up_to(sz.coarse, 128) // 128):
                    width = min(128, sz.coarse - 128 * k)
                    at = (iota((sz.block, 128), 1) + 128 * k).astype(F32)
                    pm[here, 128 * k:128 * k + width] = (at == col).astype(F32).astype(BF16)[:, 0:width]
            loads["inv"].wait()
            pa[...] = dot(pm[...], inv[...]).astype(BF16)
            ae[0:sz.rows, :] = dot(pa[...], pm[...], (1, 1)).astype(BF16)
            ae[sz.rows:sz.rows + g_rows, :] = dot(ae[sz.rows:sz.rows + g_rows, :], ae[0:sz.rows, :]).astype(BF16)

        total(hn.at[it], h_send.at[it], h_recv.at[it]).wait_recv()

        def local_jump(f):
            jump = (signs[f] * masks[f]) * (loc[face * f:face * f + face, :] - hn[it, f].astype(F32))
            if f % 2:
                wl[f // 2] = jump
            if not last:
                ml[f] = (0.25 * masks[f]) * dot(ksum[f], jump.astype(BF16))

        for f in (1, 3, 5) if last else range(6):
            local_jump(f)

        total(sx.at[it, pl.ds(0, sz.lines - 1)], sx_send.at[it], sx_recv.at[it]).wait_recv()
        packed = jnp.sum(sx[it], axis=0)
        ss[it, 1] = packed
        sy[it, l] = packed
        for dl in lanes:
            send(ss.at[it, 1], sy.at[it, l], sy_send.at[it], sy_recv.at[it], along(dl))

        total(lev.at[it, 0, pl.ds(0, nz - 1)], z_send.at[it], z_recv.at[it]).wait_recv()
        piece = lev.at[it, core]
        send(piece, piece, pp_send.at[it], pp_recv.at[it], partner)
        total(piece, pp_send.at[it], pp_recv.at[it]).wait_recv()

        for z in range(1, nz):
            level = lev[it, 0, z].astype(F32) + lev[it, 1, z - 1].astype(F32)
            bmat[sz.block * (z - 1):sz.block * z, :] = level.astype(BF16)
        sol = dot(ae[...], bmat[...])
        coarse_part = jnp.sum(sol[0:sz.rows] * bmat[...].astype(F32), axis=0, keepdims=True)
        near = sol[sz.rows:]
        near_hi = near.astype(BF16)
        near_lo = (near - near_hi.astype(F32)).astype(BF16)

        total(sy.at[it, pl.ds(0, nz - 1)], sy_send.at[it], sy_recv.at[it]).wait_recv()
        sums_now = jnp.sum(sy[it], axis=0)
        gamma, cross, delta = sums_now[0:1], sums_now[1:2], sums_now[2:3] + coarse_part
        if it == 0:
            curve = delta
        else:
            beta = gamma / gamma_old
            curve = delta + 2.0 * beta * cross + beta * beta * curve
        alpha = gamma / curve
        gamma_old = gamma

        for f in (1, 3, 5) if last else range(6):
            rows = slice(32 * (f + 1), 32 * (f + 2))
            cols = jnp.concatenate([near_hi[0:32], near_hi[rows], near_lo[0:32], near_lo[rows]], axis=0)
            a = f // 2
            if last:
                new = wl[a] + dot(wg[f, 0:face, :], cols) + beta * s[a]
                res = r[a] - alpha * new
                sum_p = u[now, f] + beta * p[a]
                r[a] = res
                x[a] = x[a] + alpha * sum_p
                continue
            both = dot(wg[f], cols)
            turned = ml[f] + both[tall:tall + face]
            if it:
                turned = turned + beta * t[f]
            t[f] = turned
            u[then, f] = u[now, f] - alpha * turned
            if f % 2:
                new = wl[a] + both[0:face]
                s[a] = new if it == 0 else new + beta * s[a]

    for copy in sent:
        copy.wait_send()
    total(idr.at[pl.ds(0, sz.lines - 1)], id_send, id_recv).wait_send()
    total(idz.at[pl.ds(0, nz - 1)], idz_send, idz_recv).wait_send()
    for it in range(ITERS):
        total(rxy.at[it, pl.ds(0, sz.lines - 1)], xy_send.at[it], xy_recv.at[it]).wait_send()
        total(sx.at[it, pl.ds(0, sz.lines - 1)], sx_send.at[it], sx_recv.at[it]).wait_send()
        total(sy.at[it, pl.ds(0, nz - 1)], sy_send.at[it], sy_recv.at[it]).wait_send()
        total(lev.at[it, 0, pl.ds(0, nz - 1)], z_send.at[it], z_recv.at[it]).wait_send()
        total(lev.at[it, 0], pp_send.at[it], pp_recv.at[it]).wait_send()
        total(hn.at[it], h_send.at[it], h_recv.at[it]).wait_send()


def deliver(face, x, r, x_h, r_h, sem):
    outs = []
    for a in range(3):
        for n, (src, dst) in enumerate(((x, x_h), (r, r_h))):
            copy = pltpu.make_async_copy(src.at[a], dst.at[pl.ds(face * a, face), 0], sem.at[n, a])
            copy.start()
            outs.append(copy)
    for copy in outs:
        copy.wait()


def body(sz, dual_rhs, local_flex, corner_coupling, face_stiffness, coarse_inverse, corner_ids):
    nx, ny, nz = sz.grid
    face, dofs, cases = sz.face, sz.dofs, sz.cases
    vmem, dma = pltpu.VMEM, pltpu.SemaphoreType.DMA
    g_rows = 7 * 32
    it = ITERS
    scratch = [
        pltpu.SMEM((8,), jnp.int32), vmem((3, face, cases), F32), vmem((dofs, dofs), BF16), vmem((24, dofs), BF16),
        vmem((6, face, face), BF16), vmem((sz.coarse, sz.coarse), BF16),
        vmem((sz.block, sz.lines * 16), BF16), vmem((sz.names, sz.lines * 8), BF16), vmem((32, 24), BF16),
        vmem((3, face, cases), BF16), vmem((3, face, cases), BF16),
        vmem((3, face, cases), BF16), vmem((3, face, cases), BF16),
        vmem((6, face, sz.split), BF16), vmem((6, sz.rest, 128), BF16), vmem((6, sz.rest, 128), BF16),
        vmem((32, sz.wide), BF16), vmem((6, 32, face), BF16), vmem((6, 32, sz.window), BF16),
        vmem((sz.wide, 128), F32), vmem((sz.window, 128), F32), vmem((6, face, face), BF16),
        vmem((6, 2 * sz.tall, 128), BF16),
        vmem((3, face, cases), F32), vmem((6, face, cases), F32),
        vmem((2, 6, face, cases), F32), vmem((3, face, cases), F32),
        vmem((dofs, cases), F32), vmem((dofs, cases), BF16), vmem((dofs, cases), F32),
        vmem((3, face, cases), F32), vmem((6, face, cases), F32),
        vmem((it, 2, 16, cases), BF16), vmem((it, sz.lines, 16, cases), BF16),
        vmem((it, 2, nz, sz.block, cases), BF16), vmem((it, 6, face, cases), BF16),
        vmem((it, 6, face, cases), BF16), vmem((sz.rows, cases), BF16),
        vmem((sz.rows + g_rows, sz.rows), BF16), vmem((sz.rows, sz.coarse), BF16),
        vmem((sz.rows, sz.coarse), BF16),
        vmem((8, cases), BF16), vmem((sz.lines, 8, cases), BF16), vmem((nz, sz.names, cases), BF16),
        vmem((it, 2, 4, cases), F32), vmem((it, sz.lines, 4, cases), F32), vmem((it, nz, 4, cases), F32),
        dma((16,)), dma((24,)), dma((6,)), dma((6,)), dma((3,)), dma((3,)), dma((6,)),
        dma, dma, dma, dma,
    ] + [dma((it,)) for _ in range(12)]
    anywhere = pl.BlockSpec(memory_space=pl.ANY)
    whole = pl.BlockSpec(memory_space=pltpu.VMEM)
    held = pltpu.VMEM((3, face, cases), F32)
    out = jax.ShapeDtypeStruct((3 * face, 1, cases), F32)
    x, res = pl.pallas_call(
        functools.partial(kernel, sz),
        out_shape=(held, held),
        in_specs=[anywhere] * 9,
        out_specs=(whole, whole),
        scratch_shapes=scratch,
        compiler_params=pltpu.CompilerParams(
            collective_id=0, has_side_effects=True, vmem_limit_bytes=56 * 1024 * 1024
        ),
        name="dual_cg",
    )(
        corner_ids.reshape(8), dual_rhs.reshape(3 * face, 1, cases), local_flex.reshape(dofs, dofs),
        corner_coupling.reshape(24, dofs), face_stiffness.reshape(6, face, face), coarse_inverse,
        *(jnp.asarray(table, BF16) for table in (*plane_sums(sz), corner_order())),
    )
    x, res = pl.pallas_call(
        functools.partial(deliver, face),
        out_shape=(out, out),
        in_specs=[whole, whole],
        out_specs=(anywhere, anywhere),
        scratch_shapes=[dma((2, 3))],
        name="deliver",
    )(*(pltpu.with_memory_space_constraint(v, pltpu.VMEM) for v in (x, res)))
    shape = (1, 1, 1, 3, face, cases)
    return x.reshape(shape), res.reshape(shape)


def solution(mesh):
    grid = (mesh.shape["gx"], mesh.shape["gy"], mesh.shape["gz"])

    def run(dual_rhs, local_flex, corner_coupling, face_stiffness, coarse_inverse, corner_ids):
        sz = Sizes(grid, dual_rhs.shape[4], dual_rhs.shape[5], coarse_inverse.shape[0])
        deep = P("gx", "gy", "gz", None, None, None)
        mid = P("gx", "gy", "gz", None, None)
        return jax.shard_map(
            functools.partial(body, sz),
            mesh=mesh,
            in_specs=(deep, mid, mid, deep, P(), P("gx", "gy", "gz", None)),
            out_specs=(deep, deep),
            check_vma=False,
        )(dual_rhs, local_flex, corner_coupling, face_stiffness, coarse_inverse, corner_ids)

    return run
```

```python
import functools

import jax
import jax.numpy as jnp
import numpy as np
from jax import lax
from jax.experimental import pallas as pl
from jax.experimental.pallas import tpu as pltpu
from jax.sharding import PartitionSpec as P

ITERS = 3
MESH = pl.DeviceIdType.MESH
F32 = jnp.float32
BF16 = jnp.bfloat16


def up_to(value, step):
    return -(-value // step) * step


def iota(shape, dim):
    return lax.broadcasted_iota(jnp.int32, shape, dim)


def dot(left, right, contract=None):
    if contract is None:
        contract = (left.ndim - 1, 0)
    dims = (((contract[0],), (contract[1],)), ((), ()))
    return lax.dot_general(left, right, dims, preferred_element_type=F32)


class Sizes:
    def __init__(self, grid, face, cases, coarse):
        self.grid, self.face, self.cases, self.coarse = grid, face, cases, coarse
        self.dofs = 6 * face
        self.window = up_to(face + 127, 128)
        self.wide = max(up_to(self.dofs, 128), face * 5 // 128 * 128 + self.window)
        self.split = face // 128 * 128
        self.rest = face - self.split
        self.tall = up_to(face, 16)
        nx, ny, nz = grid
        self.plane = (nx - 1) * (ny - 1)
        self.block = up_to(3 * self.plane + 1, 16)
        self.names = up_to(self.plane, 16)
        self.rows = up_to(self.block * (nz - 1), 128)
        self.lines = nx * ny


def plane_sums(sz):
    nx, ny, _ = sz.grid
    table = np.zeros((sz.block, sz.lines * 16), np.float32)
    names = np.zeros((sz.names, sz.lines * 8), np.float32)
    for i in range(nx):
        for j in range(ny):
            first = (i * ny + j) * 16
            for kx in range(2):
                for ky in range(2):
                    x, y = i + kx, j + ky
                    if not (1 <= x < nx and 1 <= y < ny):
                        continue
                    spot = (x - 1) * (ny - 1) + y - 1
                    for d in range(3):
                        table[d * sz.plane + spot, first + (kx * 2 + ky) * 3 + d] = 1
            if i + 1 < nx and j + 1 < ny:
                names[i * (ny - 1) + j, first // 2] = 1
    return table, names


def corner_order():
    table = np.zeros((32, 24), np.float32)
    for kx in range(2):
        for ky in range(2):
            for kz in range(2):
                for d in range(3):
                    row = kz * 16 + (kx * 2 + ky) * 3 + d
                    table[row, 3 * (4 * kx + 2 * ky + kz) + d] = 1
    return table


def kernel(sz, ids_h, rhs_h, flex_h, coup_h, stiff_h, inv_h, sums_h, sums_n_h, order_h,
           x, r,
           ids, rhs, flex, coup, stiff, inv, sums, sums_n, order,
           rhs_b, rhs_n, t_b, t_n, kn, kc, kc_n, cs, cf, cn, own_t, nb_t, ksum, wg,
           s, t, u, p, sg, sgb, loc, wl, ml, cpb, rxy, lev, hb, hn, bmat, ae, pm, pa,
           idb, idr, idz, ss, sx, sy,
           load_sem, i_send, k_recv, kc_recv, r_recv, t_recv, c_recv,
           id_send, id_recv, idz_send, idz_recv,
           xy_send, xy_recv, z_send, z_recv, pp_send, pp_recv, h_send, h_recv,
           sx_send, sx_recv, sy_send, sy_recv):
    nx, ny, nz = sz.grid
    face, dofs, split, rest, tall = sz.face, sz.dofs, sz.split, sz.rest, sz.tall
    i, j, l = lax.axis_index("gx"), lax.axis_index("gy"), lax.axis_index("gz")
    core = lax.rem(i, 2)
    place = (i, j, l)
    partner = {"gx": i + 1 - 2 * core, "gy": j, "gz": l}

    def toward(f):
        axis, step = f // 2, f % 2
        size = sz.grid[axis]
        spot = list(place)
        spot[axis] = lax.rem(spot[axis] + (1 if step else size - 1), size)
        return dict(zip(("gx", "gy", "gz"), spot))

    spread = sorted(
        [(di, dj) for di in range(nx) for dj in range(ny) if di or dj],
        key=lambda o: -(min(o[0], nx - o[0]) / 2 + min(o[1], ny - o[1])),
    )
    lanes = sorted(range(1, nz), key=lambda o: -min(o, nz - o))

    def across(di, dj):
        return {"gx": lax.rem(i + di, nx), "gy": lax.rem(j + dj, ny), "gz": l}

    def along(dl):
        return {"gx": i, "gy": j, "gz": lax.rem(l + dl, nz)}

    def remote(src, dst, send, recv, target):
        return pltpu.make_async_remote_copy(
            src_ref=src, dst_ref=dst, send_sem=send, recv_sem=recv,
            device_id=target, device_id_type=MESH,
        )

    def total(piece, send_sem, recv_sem):
        return remote(piece, piece, send_sem, recv_sem, partner)

    def send(src, dst, send_sem, recv_sem, target):
        copy = remote(src, dst, send_sem, recv_sem, target)
        copy.start()
        return copy

    loads = {}

    def load(name, src, dst):
        copy = pltpu.make_async_copy(src, dst, load_sem.at[len(loads)])
        copy.start()
        loads[name] = copy

    load("ids", ids_h, ids)
    for a in range(3):
        load(("rhs", a), rhs_h.at[pl.ds(face * a, face), 0], rhs.at[a])
    for f in (1, 3, 5, 0, 2, 4):
        load(("stiff", f), stiff_h.at[f], stiff.at[f])
    load("coup", coup_h, coup)
    load("order", order_h, order)
    load("sums", sums_h, sums)
    load("sums_n", sums_n_h, sums_n)
    load("flex", flex_h, flex)
    load("inv", inv_h, inv)

    barrier = pltpu.get_barrier_semaphore()
    for di, dj in spread:
        pl.semaphore_signal(barrier, inc=1, device_id=across(di, dj), device_id_type=MESH)
    for dl in lanes:
        pl.semaphore_signal(barrier, inc=1, device_id=along(dl), device_id_type=MESH)

    masks = []
    for f in range(6):
        axis, step = f // 2, f % 2
        edge = place[axis] < sz.grid[axis] - 1 if step else place[axis] > 0
        masks.append(jnp.where(edge, 1.0, 0.0).astype(F32))
    signs = [-1.0, 1.0] * 3

    for a in range(3):
        loads["rhs", a].wait()
        rhs_b[a] = rhs[a].astype(BF16)
        r[a] = rhs[a] * masks[2 * a + 1]
    for a in range(3):
        loads["stiff", 2 * a + 1].wait()
        t_b[a] = dot(stiff[2 * a + 1], rhs_b[a]).astype(BF16)
    kc[...] = jnp.zeros_like(kc)
    for f in (0, 2, 4, 1, 3, 5):
        if f % 2 == 0:
            loads["stiff", f].wait()
        kc[f, :, 0:rest] = stiff[f, split:face, split:face]
    loads["ids"].wait()
    idb[...] = jnp.full((8, sz.cases), ids[7], jnp.int32).astype(F32).astype(BF16)

    pl.semaphore_wait(barrier, len(spread) + len(lanes))

    sent = []

    def send_stiff(f):
        g = f ^ 1
        sent.append(send(stiff.at[f, :, pl.ds(0, split)], kn.at[g], i_send.at[f], k_recv.at[g], toward(f)))
        sent.append(send(kc.at[f], kc_n.at[g], i_send.at[6 + f], kc_recv.at[g], toward(f)))

    for a in range(3):
        sent.append(send(rhs_b.at[a], rhs_n.at[a], i_send.at[12 + a], r_recv.at[a], toward(2 * a + 1)))
        send_stiff(2 * a)
    for a in range(3):
        sent.append(send(t_b.at[a], t_n.at[a], i_send.at[15 + a], t_recv.at[a], toward(2 * a + 1)))
    slot = i * ny + j
    for di, dj in spread:
        send(idb, idr.at[slot], id_send, id_recv, across(di, dj))
    idr[slot] = idb[...]

    loads["coup"].wait()
    loads["order"].wait()
    cs[...] = jnp.zeros_like(cs)
    cs[:, 0:dofs] = dot(order[...], coup[...]).astype(BF16)
    starts = [face * f // 128 * 128 for f in range(6)]
    for f in range(6):
        sent.append(
            send(cs.at[:, pl.ds(starts[f], sz.window)], cn.at[f ^ 1], i_send.at[18 + f],
                 c_recv.at[f ^ 1], toward(f))
        )
    for f in (1, 3, 5):
        send_stiff(f)
    for f in range(6):
        off = face * f - starts[f]
        near = cs[:, starts[f]:starts[f] + sz.window].astype(F32)
        cf[f] = (signs[f] * near[:, off:off + face]).astype(BF16)
    pick_row, pick_col = iota((32, 128), 0), iota((32, 128), 1)
    pick_own = ((pick_col & 63) == pick_row).astype(F32).astype(BF16)
    pick_nb = -((pick_col & 63) == pick_row + 32).astype(F32).astype(BF16)
    own_t[...] = dot(cs[...], pick_own, (0, 0))

    g_rows = 7 * 32
    line = iota((g_rows, 128), 0)
    g, kz, e = line >> 5, (line >> 4) & 1, line & 15
    third = (e * 11) >> 5
    d, kx, ky = e - 3 * third, third >> 1, third & 1

    def shift(minus, plus):
        return (g == plus).astype(jnp.int32) - (g == minus).astype(jnp.int32)

    gx = i + kx + shift(1, 2)
    gy = j + ky + shift(3, 4)
    gz = l + kz + shift(5, 6)
    inside = (e < 12) & (gx >= 1) & (gx < nx) & (gy >= 1) & (gy < ny) & (gz >= 1) & (gz < nz)
    spot = jnp.where(
        inside, sz.block * (gz - 1) + sz.plane * d + (ny - 1) * (gx - 1) + gy - 1, -1
    )
    for k in range(sz.rows // 128):
        ae[sz.rows:sz.rows + g_rows, 128 * k:128 * k + 128] = (
            (iota((g_rows, 128), 1) + 128 * k == spot).astype(F32).astype(BF16)
        )
    bmat[...] = jnp.zeros_like(bmat)
    pm[...] = jnp.zeros_like(pm)
    wg[...] = jnp.zeros_like(wg)
    eye = (iota((rest, 128), 0) == iota((rest, 128), 1)).astype(F32).astype(BF16)

    def add_stiffness(f):
        for copy in (
            remote(kn.at[f], kn.at[f], i_send.at[f], k_recv.at[f], toward(f)),
            remote(kc.at[f], kc_n.at[f], i_send.at[6 + f], kc_recv.at[f], toward(f)),
        ):
            copy.wait_recv()
        both = (stiff[f, :, 0:split].astype(F32) + kn[f].astype(F32)).astype(BF16)
        ksum[f, :, 0:split] = both
        turned = dot(both[split:face], eye, (0, 0))
        ksum[f, 0:split, split:face] = turned[:, 0:rest].astype(BF16)
        ksum[f, split:face, split:face] = (
            stiff[f, split:face, split:face].astype(F32) + kc_n[f, :, 0:rest].astype(F32)
        ).astype(BF16)

    for a in range(3):
        remote(rhs_b.at[a], rhs_n.at[a], i_send.at[12 + a], r_recv.at[a], partner).wait_recv()
        part = dot(stiff[2 * a], rhs_n[a])
        add_stiffness(2 * a + 1)
        u[0, 2 * a + 1] = (0.25 * masks[2 * a + 1]) * dot(ksum[2 * a + 1], rhs_b[a])
        remote(t_b.at[a], t_n.at[a], i_send.at[15 + a], t_recv.at[a], partner).wait_recv()
        u[0, 2 * a] = (0.25 * masks[2 * a]) * (part + t_n[a].astype(F32))

    def corner_part(value):
        part = None
        for f in range(6):
            piece = dot(cf[f], value(f).astype(BF16))
            part = piece if part is None else part + piece
        return part

    alpha = beta = gamma_old = curve = cp = cp_turned = None
    for it in range(ITERS):
        last = it + 1 == ITERS
        now, then = it % 2, (it + 1) % 2
        if it == 0:
            cp = corner_part(lambda f: u[0, f])
        low, high = cp[0:16].astype(BF16), cp[16:32].astype(BF16)
        cpb[it, 0] = low
        cpb[it, 1] = high
        for di, dj in spread:
            target = across(di, dj)
            send(cpb.at[it, lax.rem(target["gx"], 2)], rxy.at[it, slot], xy_send.at[it],
                 xy_recv.at[it], target)
        rxy[it, slot] = jnp.where(core == 0, low.astype(F32), high.astype(F32)).astype(BF16)
        if it == 0:
            total(idr.at[pl.ds(0, sz.lines - 1)], id_send, id_recv).wait_recv()
            loads["sums"].wait()
            loads["sums_n"].wait()
            idz[l] = dot(sums_n[...], idr[...].reshape(sz.lines * 8, sz.cases)).astype(BF16)
            for dl in lanes:
                send(idz.at[l], idz.at[l], idz_send, idz_recv, along(dl))

        for f in range(6):
            if it:
                t[f] = ml[f] if it == 1 else ml[f] + beta * t[f]
                u[now, f] = u[then, f] - alpha * t[f]
            sg[face * f:face * f + face, :] = signs[f] * u[now, f]
        sgb[...] = sg[...].astype(BF16)
        if it == 0:
            loads["flex"].wait()
        loc[...] = dot(flex[...], sgb[...])
        delta = jnp.sum(sgb[...].astype(F32) * loc[...], axis=0, keepdims=True)
        if it:
            for a in range(3):
                s[a] = wl[a] if it == 1 else wl[a] + beta * s[a]
                r[a] = r[a] - alpha * s[a]
        gamma = sum(jnp.sum(r[a] * u[now, 2 * a + 1], axis=0, keepdims=True) for a in range(3))
        if it:
            cross = sum(jnp.sum(s[a] * u[now, 2 * a + 1], axis=0, keepdims=True) for a in range(3))
        else:
            cross = jnp.zeros_like(gamma)
        where = iota((4, sz.cases), 0)
        packed = jnp.where(where == 0, gamma, jnp.where(where == 1, cross, jnp.where(where == 2, delta, 0.0)))
        ss[it, 0] = packed
        sx[it, slot] = packed
        for di, dj in spread:
            send(ss.at[it, 0], sx.at[it, slot], sx_send.at[it], sx_recv.at[it], across(di, dj))
        for f in (0, 2, 4) if last else range(6):
            hb[it, f] = loc[face * f:face * f + face, :].astype(BF16)
            send(hb.at[it, f], hn.at[it, f ^ 1], h_send.at[it], h_recv.at[it], toward(f))
        if it:
            for a in range(3):
                new = u[then, 2 * a + 1]
                if it > 1:
                    new = new + beta * p[a]
                p[a] = new
                x[a] = alpha * new if it == 1 else x[a] + alpha * new

        if it == 0:
            for f in (0, 2, 4):
                add_stiffness(f)
            for f in range(6):
                remote(cs.at[:, pl.ds(starts[f], sz.window)], cn.at[f], i_send.at[18 + f],
                       c_recv.at[f], toward(f)).wait_recv()
                nb_t[...] = dot(cn[f], pick_nb, (0, 0))
                off = face * (f ^ 1) - starts[f ^ 1]
                wide = (signs[f] * masks[f]) * (own_t[face * f:face * f + face, :] + nb_t[off:off + face, :])
                wide = wide.astype(BF16)
                wg[f, 0:face, :] = wide
                wg[f, tall:tall + face, :] = ((0.25 * masks[f]) * dot(ksum[f], wide)).astype(BF16)

        total(rxy.at[it, pl.ds(0, sz.lines - 1)], xy_send.at[it], xy_recv.at[it]).wait_recv()
        lev[it, core, l] = dot(sums[...], rxy[it].reshape(sz.lines * 16, sz.cases)).astype(BF16)
        for dl in lanes:
            piece = lev.at[it, core, l]
            send(piece, piece, z_send.at[it], z_recv.at[it], along(dl))

        total(hn.at[it, pl.ds(0, 3)] if last else hn.at[it], h_send.at[it], h_recv.at[it]).wait_recv()

        def local_jump(f):
            jump = (signs[f] * masks[f]) * (loc[face * f:face * f + face, :] - hn[it, f].astype(F32))
            if f % 2:
                wl[f // 2] = jump
            if not last:
                ml[f] = (0.25 * masks[f]) * dot(ksum[f], jump.astype(BF16))

        for f in (1, 3, 5) if last else range(6):
            local_jump(f)

        total(sx.at[it, pl.ds(0, sz.lines - 1)], sx_send.at[it], sx_recv.at[it]).wait_recv()
        packed = jnp.sum(sx[it], axis=0)
        ss[it, 1] = packed
        sy[it, l] = packed
        for dl in lanes:
            send(ss.at[it, 1], sy.at[it, l], sy_send.at[it], sy_recv.at[it], along(dl))

        if it == 0:
            small_r, small_c = iota((sz.block, sz.names), 0), iota((sz.block, sz.names), 1)
            part = (small_r >= sz.plane).astype(jnp.int32) + (small_r >= 2 * sz.plane).astype(jnp.int32)
            expand = ((small_c == small_r - sz.plane * part) & (small_r < 3 * sz.plane)).astype(F32).astype(BF16)
            rr = iota((sz.block, 128), 0)
            comp = (rr >= sz.plane).astype(jnp.int32) + (rr >= 2 * sz.plane).astype(jnp.int32)
            total(idz.at[pl.ds(0, nz - 1)], idz_send, idz_recv).wait_recv()
            for z in range(1, nz):
                here = pl.ds(sz.block * (z - 1), sz.block)
                col = 3.0 * dot(expand, idz[z - 1]) + comp.astype(F32)
                col = jnp.where(rr < 3 * sz.plane, col, -1.0)
                for k in range(up_to(sz.coarse, 128) // 128):
                    width = min(128, sz.coarse - 128 * k)
                    at = (iota((sz.block, 128), 1) + 128 * k).astype(F32)
                    pm[here, 128 * k:128 * k + width] = (at == col).astype(F32).astype(BF16)[:, 0:width]
            loads["inv"].wait()
            pa[...] = dot(pm[...], inv[...]).astype(BF16)
            ae[0:sz.rows, :] = dot(pa[...], pm[...], (1, 1)).astype(BF16)
            ae[sz.rows:sz.rows + g_rows, :] = dot(ae[sz.rows:sz.rows + g_rows, :], ae[0:sz.rows, :]).astype(BF16)

        total(lev.at[it, 0, pl.ds(0, nz - 1)], z_send.at[it], z_recv.at[it]).wait_recv()
        piece = lev.at[it, core]
        send(piece, piece, pp_send.at[it], pp_recv.at[it], partner)
        total(piece, pp_send.at[it], pp_recv.at[it]).wait_recv()

        for z in range(1, nz):
            level = lev[it, 0, z].astype(F32) + lev[it, 1, z - 1].astype(F32)
            bmat[sz.block * (z - 1):sz.block * z, :] = level.astype(BF16)
        sol = dot(ae[...], bmat[...])
        coarse_part = jnp.sum(sol[0:sz.rows] * bmat[...].astype(F32), axis=0, keepdims=True)
        near = sol[sz.rows:]
        near_hi = near.astype(BF16)
        near_lo = (near - near_hi.astype(F32)).astype(BF16)

        def columns(f):
            rows = slice(32 * (f + 1), 32 * (f + 2))
            return jnp.concatenate([near_hi[0:32], near_hi[rows], near_lo[0:32], near_lo[rows]], axis=0)

        if last:
            for a in range(3):
                f = 2 * a + 1
                wl[a] = wl[a] + dot(wg[f, 0:face, :], columns(f))
        else:
            for f in range(6):
                both = dot(wg[f], columns(f))
                ml[f] = ml[f] + both[tall:tall + face]
                if f % 2:
                    wl[f // 2] = wl[f // 2] + both[0:face]
            turned = corner_part(lambda f: ml[f])
        total(sy.at[it, pl.ds(0, nz - 1)], sy_send.at[it], sy_recv.at[it]).wait_recv()
        sums_now = jnp.sum(sy[it], axis=0)
        gamma, cross, delta = sums_now[0:1], sums_now[1:2], sums_now[2:3] + coarse_part
        if it == 0:
            curve = delta
        else:
            beta = gamma / gamma_old
            curve = delta + 2.0 * beta * cross + beta * beta * curve
        alpha = gamma / curve
        gamma_old = gamma

        if last:
            for a in range(3):
                r[a] = r[a] - alpha * (wl[a] + beta * s[a])
                x[a] = x[a] + alpha * (u[now, 2 * a + 1] + beta * p[a])
        else:
            cp_turned = turned if it == 0 else turned + beta * cp_turned
            cp = cp - alpha * cp_turned

    for copy in sent:
        copy.wait_send()
    total(idr.at[pl.ds(0, sz.lines - 1)], id_send, id_recv).wait_send()
    total(idz.at[pl.ds(0, nz - 1)], idz_send, idz_recv).wait_send()
    for it in range(ITERS):
        total(rxy.at[it, pl.ds(0, sz.lines - 1)], xy_send.at[it], xy_recv.at[it]).wait_send()
        total(sx.at[it, pl.ds(0, sz.lines - 1)], sx_send.at[it], sx_recv.at[it]).wait_send()
        total(sy.at[it, pl.ds(0, nz - 1)], sy_send.at[it], sy_recv.at[it]).wait_send()
        total(lev.at[it, 0, pl.ds(0, nz - 1)], z_send.at[it], z_recv.at[it]).wait_send()
        total(lev.at[it, 0], pp_send.at[it], pp_recv.at[it]).wait_send()
        part = hn.at[it, pl.ds(0, 3)] if it + 1 == ITERS else hn.at[it]
        total(part, h_send.at[it], h_recv.at[it]).wait_send()


def deliver(face, x, r, x_h, r_h, sem):
    outs = []
    for a in range(3):
        for n, (src, dst) in enumerate(((x, x_h), (r, r_h))):
            copy = pltpu.make_async_copy(src.at[a], dst.at[pl.ds(face * a, face), 0], sem.at[n, a])
            copy.start()
            outs.append(copy)
    for copy in outs:
        copy.wait()


def body(sz, dual_rhs, local_flex, corner_coupling, face_stiffness, coarse_inverse, corner_ids):
    nx, ny, nz = sz.grid
    face, dofs, cases = sz.face, sz.dofs, sz.cases
    vmem, dma = pltpu.VMEM, pltpu.SemaphoreType.DMA
    g_rows = 7 * 32
    it = ITERS
    scratch = [
        pltpu.SMEM((8,), jnp.int32), vmem((3, face, cases), F32), vmem((dofs, dofs), BF16), vmem((24, dofs), BF16),
        vmem((6, face, face), BF16), vmem((sz.coarse, sz.coarse), BF16),
        vmem((sz.block, sz.lines * 16), BF16), vmem((sz.names, sz.lines * 8), BF16), vmem((32, 24), BF16),
        vmem((3, face, cases), BF16), vmem((3, face, cases), BF16),
        vmem((3, face, cases), BF16), vmem((3, face, cases), BF16),
        vmem((6, face, sz.split), BF16), vmem((6, sz.rest, 128), BF16), vmem((6, sz.rest, 128), BF16),
        vmem((32, sz.wide), BF16), vmem((6, 32, face), BF16), vmem((6, 32, sz.window), BF16),
        vmem((sz.wide, 128), F32), vmem((sz.window, 128), F32), vmem((6, face, face), BF16),
        vmem((6, 2 * sz.tall, 128), BF16),
        vmem((3, face, cases), F32), vmem((6, face, cases), F32),
        vmem((2, 6, face, cases), F32), vmem((3, face, cases), F32),
        vmem((dofs, cases), F32), vmem((dofs, cases), BF16), vmem((dofs, cases), F32),
        vmem((3, face, cases), F32), vmem((6, face, cases), F32),
        vmem((it, 2, 16, cases), BF16), vmem((it, sz.lines, 16, cases), BF16),
        vmem((it, 2, nz, sz.block, cases), BF16), vmem((it, 6, face, cases), BF16),
        vmem((it, 6, face, cases), BF16), vmem((sz.rows, cases), BF16),
        vmem((sz.rows + g_rows, sz.rows), BF16), vmem((sz.rows, sz.coarse), BF16),
        vmem((sz.rows, sz.coarse), BF16),
        vmem((8, cases), BF16), vmem((sz.lines, 8, cases), BF16), vmem((nz, sz.names, cases), BF16),
        vmem((it, 2, 4, cases), F32), vmem((it, sz.lines, 4, cases), F32), vmem((it, nz, 4, cases), F32),
        dma((16,)), dma((24,)), dma((6,)), dma((6,)), dma((3,)), dma((3,)), dma((6,)),
        dma, dma, dma, dma,
    ] + [dma((it,)) for _ in range(12)]
    anywhere = pl.BlockSpec(memory_space=pl.ANY)
    whole = pl.BlockSpec(memory_space=pltpu.VMEM)
    held = pltpu.VMEM((3, face, cases), F32)
    out = jax.ShapeDtypeStruct((3 * face, 1, cases), F32)
    x, res = pl.pallas_call(
        functools.partial(kernel, sz),
        out_shape=(held, held),
        in_specs=[anywhere] * 9,
        out_specs=(whole, whole),
        scratch_shapes=scratch,
        compiler_params=pltpu.CompilerParams(
            collective_id=0, has_side_effects=True, vmem_limit_bytes=56 * 1024 * 1024
        ),
        name="dual_cg",
    )(
        corner_ids.reshape(8), dual_rhs.reshape(3 * face, 1, cases), local_flex.reshape(dofs, dofs),
        corner_coupling.reshape(24, dofs), face_stiffness.reshape(6, face, face), coarse_inverse,
        *(jnp.asarray(table, BF16) for table in (*plane_sums(sz), corner_order())),
    )
    x, res = pl.pallas_call(
        functools.partial(deliver, face),
        out_shape=(out, out),
        in_specs=[whole, whole],
        out_specs=(anywhere, anywhere),
        scratch_shapes=[dma((2, 3))],
        name="deliver",
    )(*(pltpu.with_memory_space_constraint(v, pltpu.VMEM) for v in (x, res)))
    shape = (1, 1, 1, 3, face, cases)
    return x.reshape(shape), res.reshape(shape)


def solution(mesh):
    grid = (mesh.shape["gx"], mesh.shape["gy"], mesh.shape["gz"])

    def run(dual_rhs, local_flex, corner_coupling, face_stiffness, coarse_inverse, corner_ids):
        sz = Sizes(grid, dual_rhs.shape[4], dual_rhs.shape[5], coarse_inverse.shape[0])
        deep = P("gx", "gy", "gz", None, None, None)
        mid = P("gx", "gy", "gz", None, None)
        return jax.shard_map(
            functools.partial(body, sz),
            mesh=mesh,
            in_specs=(deep, mid, mid, deep, P(), P("gx", "gy", "gz", None)),
            out_specs=(deep, deep),
            check_vma=False,
        )(dual_rhs, local_flex, corner_coupling, face_stiffness, coarse_inverse, corner_ids)

    return run
```

```python
import functools

import jax
import jax.numpy as jnp
import numpy as np
from jax import lax
from jax.experimental import pallas as pl
from jax.experimental.pallas import tpu as pltpu
from jax.sharding import PartitionSpec as P

ITERS = 3
MESH = pl.DeviceIdType.MESH
F32 = jnp.float32
BF16 = jnp.bfloat16


def up_to(value, step):
    return -(-value // step) * step


def iota(shape, dim):
    return lax.broadcasted_iota(jnp.int32, shape, dim)


def dot(left, right, contract=None):
    if contract is None:
        contract = (left.ndim - 1, 0)
    dims = (((contract[0],), (contract[1],)), ((), ()))
    return lax.dot_general(left, right, dims, preferred_element_type=F32)


class Sizes:
    def __init__(self, grid, face, cases, coarse):
        self.grid, self.face, self.cases, self.coarse = grid, face, cases, coarse
        self.dofs = 6 * face
        self.window = up_to(face + 127, 128)
        self.wide = max(up_to(self.dofs, 128), face * 5 // 128 * 128 + self.window)
        self.split = face // 128 * 128
        self.rest = face - self.split
        self.tall = up_to(face, 16)
        nx, ny, nz = grid
        self.plane = (nx - 1) * (ny - 1)
        self.block = up_to(3 * self.plane + 1, 16)
        self.names = up_to(self.plane, 16)
        self.rows = up_to(self.block * (nz - 1), 128)
        self.lines = nx * ny


def plane_sums(sz):
    nx, ny, _ = sz.grid
    table = np.zeros((sz.block, sz.lines * 16), np.float32)
    names = np.zeros((sz.names, sz.lines * 8), np.float32)
    for i in range(nx):
        for j in range(ny):
            first = (i * ny + j) * 16
            for kx in range(2):
                for ky in range(2):
                    x, y = i + kx, j + ky
                    if not (1 <= x < nx and 1 <= y < ny):
                        continue
                    spot = (x - 1) * (ny - 1) + y - 1
                    for d in range(3):
                        table[d * sz.plane + spot, first + (kx * 2 + ky) * 3 + d] = 1
            if i + 1 < nx and j + 1 < ny:
                names[i * (ny - 1) + j, first // 2] = 1
    return table, names


def corner_order():
    table = np.zeros((32, 24), np.float32)
    for kx in range(2):
        for ky in range(2):
            for kz in range(2):
                for d in range(3):
                    row = kz * 16 + (kx * 2 + ky) * 3 + d
                    table[row, 3 * (4 * kx + 2 * ky + kz) + d] = 1
    return table


def kernel(sz, ids_h, rhs_h, flex_h, coup_h, stiff_h, inv_h, sums_h, sums_n_h, order_h,
           x, r,
           ids, rhs, flex, coup, stiff, inv, sums, sums_n, order,
           rhs_b, rhs_n, t_b, t_n, kn, kc, kc_n, cs, cf, cn, own_t, nb_t, ksum, wg,
           s, t, u, p, sg, sgb, loc, wl, ml, cpb, rxy, lev, hb, hn, bmat, ae, pm, pa,
           idb, idr, idz, ss, sx, sy,
           load_sem, i_send, k_recv, kc_recv, r_recv, t_recv, c_recv,
           id_send, id_recv, idz_send, idz_recv,
           xy_send, xy_recv, z_send, z_recv, pp_send, pp_recv, h_send, h_recv,
           sx_send, sx_recv, sy_send, sy_recv):
    nx, ny, nz = sz.grid
    face, dofs, split, rest, tall = sz.face, sz.dofs, sz.split, sz.rest, sz.tall
    i, j, l = lax.axis_index("gx"), lax.axis_index("gy"), lax.axis_index("gz")
    core = lax.rem(i, 2)
    place = (i, j, l)
    partner = {"gx": i + 1 - 2 * core, "gy": j, "gz": l}

    def toward(f):
        axis, step = f // 2, f % 2
        size = sz.grid[axis]
        spot = list(place)
        spot[axis] = lax.rem(spot[axis] + (1 if step else size - 1), size)
        return dict(zip(("gx", "gy", "gz"), spot))

    spread = sorted(
        [(di, dj) for di in range(nx) for dj in range(ny) if di or dj],
        key=lambda o: -(min(o[0], nx - o[0]) / 2 + min(o[1], ny - o[1])),
    )
    lanes = sorted(range(1, nz), key=lambda o: -min(o, nz - o))

    def across(di, dj):
        return {"gx": lax.rem(i + di, nx), "gy": lax.rem(j + dj, ny), "gz": l}

    def along(dl):
        return {"gx": i, "gy": j, "gz": lax.rem(l + dl, nz)}

    def remote(src, dst, send, recv, target):
        return pltpu.make_async_remote_copy(
            src_ref=src, dst_ref=dst, send_sem=send, recv_sem=recv,
            device_id=target, device_id_type=MESH,
        )

    def total(piece, send_sem, recv_sem):
        return remote(piece, piece, send_sem, recv_sem, partner)

    def send(src, dst, send_sem, recv_sem, target):
        copy = remote(src, dst, send_sem, recv_sem, target)
        copy.start()
        return copy

    loads = {}

    def load(name, src, dst):
        copy = pltpu.make_async_copy(src, dst, load_sem.at[len(loads)])
        copy.start()
        loads[name] = copy

    load("ids", ids_h, ids)
    for a in range(3):
        load(("rhs", a), rhs_h.at[pl.ds(face * a, face), 0], rhs.at[a])
    for f in (1, 3, 5, 0, 2, 4):
        load(("stiff", f), stiff_h.at[f], stiff.at[f])
    load("coup", coup_h, coup)
    load("order", order_h, order)
    load("sums", sums_h, sums)
    load("sums_n", sums_n_h, sums_n)
    load("flex", flex_h, flex)
    load("inv", inv_h, inv)

    barrier = pltpu.get_barrier_semaphore()
    for di, dj in spread:
        pl.semaphore_signal(barrier, inc=1, device_id=across(di, dj), device_id_type=MESH)
    for dl in lanes:
        pl.semaphore_signal(barrier, inc=1, device_id=along(dl), device_id_type=MESH)

    masks = []
    for f in range(6):
        axis, step = f // 2, f % 2
        edge = place[axis] < sz.grid[axis] - 1 if step else place[axis] > 0
        masks.append(jnp.where(edge, 1.0, 0.0).astype(F32))
    signs = [-1.0, 1.0] * 3

    for a in range(3):
        loads["rhs", a].wait()
        rhs_b[a] = rhs[a].astype(BF16)
        r[a] = rhs[a] * masks[2 * a + 1]
    for a in range(3):
        loads["stiff", 2 * a + 1].wait()
        t_b[a] = dot(stiff[2 * a + 1], rhs_b[a]).astype(BF16)
    kc[...] = jnp.zeros_like(kc)
    for f in (0, 2, 4, 1, 3, 5):
        if f % 2 == 0:
            loads["stiff", f].wait()
        kc[f, :, 0:rest] = stiff[f, split:face, split:face]
    loads["ids"].wait()
    idb[...] = jnp.full((8, sz.cases), ids[7], jnp.int32).astype(F32).astype(BF16)

    pl.semaphore_wait(barrier, len(spread) + len(lanes))

    sent = []

    def send_stiff(f):
        g = f ^ 1
        sent.append(send(stiff.at[f, :, pl.ds(0, split)], kn.at[g], i_send.at[f], k_recv.at[g], toward(f)))
        sent.append(send(kc.at[f], kc_n.at[g], i_send.at[6 + f], kc_recv.at[g], toward(f)))

    for a in range(3):
        sent.append(send(rhs_b.at[a], rhs_n.at[a], i_send.at[12 + a], r_recv.at[a], toward(2 * a + 1)))
        send_stiff(2 * a)
    for a in range(3):
        sent.append(send(t_b.at[a], t_n.at[a], i_send.at[15 + a], t_recv.at[a], toward(2 * a + 1)))
    slot = i * ny + j
    for di, dj in spread:
        send(idb, idr.at[slot], id_send, id_recv, across(di, dj))
    idr[slot] = idb[...]

    loads["coup"].wait()
    loads["order"].wait()
    cs[...] = jnp.zeros_like(cs)
    cs[:, 0:dofs] = dot(order[...], coup[...]).astype(BF16)
    starts = [face * f // 128 * 128 for f in range(6)]
    for f in range(6):
        sent.append(
            send(cs.at[:, pl.ds(starts[f], sz.window)], cn.at[f ^ 1], i_send.at[18 + f],
                 c_recv.at[f ^ 1], toward(f))
        )
    for f in (1, 3, 5):
        send_stiff(f)
    for f in range(6):
        off = face * f - starts[f]
        near = cs[:, starts[f]:starts[f] + sz.window].astype(F32)
        cf[f] = (signs[f] * near[:, off:off + face]).astype(BF16)
    pick_row, pick_col = iota((32, 128), 0), iota((32, 128), 1)
    pick_own = ((pick_col & 63) == pick_row).astype(F32).astype(BF16)
    pick_nb = -((pick_col & 63) == pick_row + 32).astype(F32).astype(BF16)
    own_t[...] = dot(cs[...], pick_own, (0, 0))

    g_rows = 7 * 32
    line = iota((g_rows, 128), 0)
    g, kz, e = line >> 5, (line >> 4) & 1, line & 15
    third = (e * 11) >> 5
    d, kx, ky = e - 3 * third, third >> 1, third & 1

    def shift(minus, plus):
        return (g == plus).astype(jnp.int32) - (g == minus).astype(jnp.int32)

    gx = i + kx + shift(1, 2)
    gy = j + ky + shift(3, 4)
    gz = l + kz + shift(5, 6)
    inside = (e < 12) & (gx >= 1) & (gx < nx) & (gy >= 1) & (gy < ny) & (gz >= 1) & (gz < nz)
    spot = jnp.where(
        inside, sz.block * (gz - 1) + sz.plane * d + (ny - 1) * (gx - 1) + gy - 1, -1
    )
    for k in range(sz.rows // 128):
        ae[sz.rows:sz.rows + g_rows, 128 * k:128 * k + 128] = (
            (iota((g_rows, 128), 1) + 128 * k == spot).astype(F32).astype(BF16)
        )
    bmat[...] = jnp.zeros_like(bmat)
    pm[...] = jnp.zeros_like(pm)
    wg[...] = jnp.zeros_like(wg)
    eye = (iota((rest, 128), 0) == iota((rest, 128), 1)).astype(F32).astype(BF16)

    def add_stiffness(f):
        for copy in (
            remote(kn.at[f], kn.at[f], i_send.at[f], k_recv.at[f], toward(f)),
            remote(kc.at[f], kc_n.at[f], i_send.at[6 + f], kc_recv.at[f], toward(f)),
        ):
            copy.wait_recv()
        both = (stiff[f, :, 0:split].astype(F32) + kn[f].astype(F32)).astype(BF16)
        ksum[f, :, 0:split] = both
        turned = dot(both[split:face], eye, (0, 0))
        ksum[f, 0:split, split:face] = turned[:, 0:rest].astype(BF16)
        ksum[f, split:face, split:face] = (
            stiff[f, split:face, split:face].astype(F32) + kc_n[f, :, 0:rest].astype(F32)
        ).astype(BF16)

    for a in range(3):
        remote(rhs_b.at[a], rhs_n.at[a], i_send.at[12 + a], r_recv.at[a], partner).wait_recv()
        part = dot(stiff[2 * a], rhs_n[a])
        add_stiffness(2 * a + 1)
        u[0, 2 * a + 1] = (0.25 * masks[2 * a + 1]) * dot(ksum[2 * a + 1], rhs_b[a])
        remote(t_b.at[a], t_n.at[a], i_send.at[15 + a], t_recv.at[a], partner).wait_recv()
        u[0, 2 * a] = (0.25 * masks[2 * a]) * (part + t_n[a].astype(F32))

    def corner_part(value):
        part = None
        for f in range(6):
            piece = dot(cf[f], value(f).astype(BF16))
            part = piece if part is None else part + piece
        return part

    alpha = beta = gamma_old = curve = cp = cp_turned = None
    for it in range(ITERS):
        last = it + 1 == ITERS
        now, then = it % 2, (it + 1) % 2
        if it == 0:
            cp = corner_part(lambda f: u[0, f])
        low, high = cp[0:16].astype(BF16), cp[16:32].astype(BF16)
        cpb[it, 0] = low
        cpb[it, 1] = high
        for di, dj in spread:
            target = across(di, dj)
            send(cpb.at[it, lax.rem(target["gx"], 2)], rxy.at[it, slot], xy_send.at[it],
                 xy_recv.at[it], target)
        rxy[it, slot] = jnp.where(core == 0, low.astype(F32), high.astype(F32)).astype(BF16)
        if it == 0:
            total(idr.at[pl.ds(0, sz.lines - 1)], id_send, id_recv).wait_recv()
            loads["sums"].wait()
            loads["sums_n"].wait()
            idz[l] = dot(sums_n[...], idr[...].reshape(sz.lines * 8, sz.cases)).astype(BF16)
            for dl in lanes:
                send(idz.at[l], idz.at[l], idz_send, idz_recv, along(dl))

        for f in range(6):
            if it:
                t[f] = ml[f] if it == 1 else ml[f] + beta * t[f]
                u[now, f] = u[then, f] - alpha * t[f]
            sg[face * f:face * f + face, :] = signs[f] * u[now, f]
        sgb[...] = sg[...].astype(BF16)
        if it == 0:
            loads["flex"].wait()
        loc[...] = dot(flex[...], sgb[...])
        delta = jnp.sum(sgb[...].astype(F32) * loc[...], axis=0, keepdims=True)
        if it:
            for a in range(3):
                s[a] = wl[a] if it == 1 else wl[a] + beta * s[a]
                r[a] = r[a] - alpha * s[a]
        gamma = sum(jnp.sum(r[a] * u[now, 2 * a + 1], axis=0, keepdims=True) for a in range(3))
        if it:
            cross = sum(jnp.sum(s[a] * u[now, 2 * a + 1], axis=0, keepdims=True) for a in range(3))
        else:
            cross = jnp.zeros_like(gamma)
        where = iota((4, sz.cases), 0)
        packed = jnp.where(where == 0, gamma, jnp.where(where == 1, cross, jnp.where(where == 2, delta, 0.0)))
        ss[it, 0] = packed
        sx[it, slot] = packed
        for di, dj in spread:
            send(ss.at[it, 0], sx.at[it, slot], sx_send.at[it], sx_recv.at[it], across(di, dj))
        for f in (0, 2, 4) if last else range(6):
            hb[it, f] = loc[face * f:face * f + face, :].astype(BF16)
            send(hb.at[it, f], hn.at[it, f ^ 1], h_send.at[it], h_recv.at[it], toward(f))
        if it:
            for a in range(3):
                new = u[then, 2 * a + 1]
                if it > 1:
                    new = new + beta * p[a]
                p[a] = new
                x[a] = alpha * new if it == 1 else x[a] + alpha * new

        if it == 0:
            for f in (0, 2, 4):
                add_stiffness(f)
            for f in range(6):
                remote(cs.at[:, pl.ds(starts[f], sz.window)], cn.at[f], i_send.at[18 + f],
                       c_recv.at[f], toward(f)).wait_recv()
                nb_t[...] = dot(cn[f], pick_nb, (0, 0))
                off = face * (f ^ 1) - starts[f ^ 1]
                wide = (signs[f] * masks[f]) * (own_t[face * f:face * f + face, :] + nb_t[off:off + face, :])
                wide = wide.astype(BF16)
                wg[f, 0:face, :] = wide
                wg[f, tall:tall + face, :] = ((0.25 * masks[f]) * dot(ksum[f], wide)).astype(BF16)

        total(rxy.at[it, pl.ds(0, sz.lines - 1)], xy_send.at[it], xy_recv.at[it]).wait_recv()
        lev[it, core, l] = dot(sums[...], rxy[it].reshape(sz.lines * 16, sz.cases)).astype(BF16)
        for dl in lanes:
            piece = lev.at[it, core, l]
            send(piece, piece, z_send.at[it], z_recv.at[it], along(dl))

        total(sx.at[it, pl.ds(0, sz.lines - 1)], sx_send.at[it], sx_recv.at[it]).wait_recv()
        packed = jnp.sum(sx[it], axis=0)
        ss[it, 1] = packed
        sy[it, l] = packed
        for dl in lanes:
            send(ss.at[it, 1], sy.at[it, l], sy_send.at[it], sy_recv.at[it], along(dl))

        total(hn.at[it, pl.ds(0, 3)] if last else hn.at[it], h_send.at[it], h_recv.at[it]).wait_recv()

        def local_jump(f):
            jump = (signs[f] * masks[f]) * (loc[face * f:face * f + face, :] - hn[it, f].astype(F32))
            if f % 2:
                wl[f // 2] = jump
            if not last:
                ml[f] = (0.25 * masks[f]) * dot(ksum[f], jump.astype(BF16))

        for f in (1, 3, 5) if last else range(6):
            local_jump(f)

        if it == 0:
            small_r, small_c = iota((sz.block, sz.names), 0), iota((sz.block, sz.names), 1)
            part = (small_r >= sz.plane).astype(jnp.int32) + (small_r >= 2 * sz.plane).astype(jnp.int32)
            expand = ((small_c == small_r - sz.plane * part) & (small_r < 3 * sz.plane)).astype(F32).astype(BF16)
            rr = iota((sz.block, 128), 0)
            comp = (rr >= sz.plane).astype(jnp.int32) + (rr >= 2 * sz.plane).astype(jnp.int32)
            total(idz.at[pl.ds(0, nz - 1)], idz_send, idz_recv).wait_recv()
            for z in range(1, nz):
                here = pl.ds(sz.block * (z - 1), sz.block)
                col = 3.0 * dot(expand, idz[z - 1]) + comp.astype(F32)
                col = jnp.where(rr < 3 * sz.plane, col, -1.0)
                for k in range(up_to(sz.coarse, 128) // 128):
                    width = min(128, sz.coarse - 128 * k)
                    at = (iota((sz.block, 128), 1) + 128 * k).astype(F32)
                    pm[here, 128 * k:128 * k + width] = (at == col).astype(F32).astype(BF16)[:, 0:width]
            loads["inv"].wait()
            pa[...] = dot(pm[...], inv[...]).astype(BF16)
            ae[0:sz.rows, :] = dot(pa[...], pm[...], (1, 1)).astype(BF16)
            ae[sz.rows:sz.rows + g_rows, :] = dot(ae[sz.rows:sz.rows + g_rows, :], ae[0:sz.rows, :]).astype(BF16)

        total(lev.at[it, 0, pl.ds(0, nz - 1)], z_send.at[it], z_recv.at[it]).wait_recv()
        piece = lev.at[it, core]
        send(piece, piece, pp_send.at[it], pp_recv.at[it], partner)
        total(piece, pp_send.at[it], pp_recv.at[it]).wait_recv()

        for z in range(1, nz):
            level = lev[it, 0, z].astype(F32) + lev[it, 1, z - 1].astype(F32)
            bmat[sz.block * (z - 1):sz.block * z, :] = level.astype(BF16)
        sol = dot(ae[...], bmat[...])
        coarse_part = jnp.sum(sol[0:sz.rows] * bmat[...].astype(F32), axis=0, keepdims=True)
        near = sol[sz.rows:]
        near_hi = near.astype(BF16)
        near_lo = (near - near_hi.astype(F32)).astype(BF16)

        def columns(f):
            rows = slice(32 * (f + 1), 32 * (f + 2))
            return jnp.concatenate([near_hi[0:32], near_hi[rows], near_lo[0:32], near_lo[rows]], axis=0)

        if last:
            for a in range(3):
                f = 2 * a + 1
                wl[a] = wl[a] + dot(wg[f, 0:face, :], columns(f))
        else:
            for f in range(6):
                both = dot(wg[f], columns(f))
                ml[f] = ml[f] + both[tall:tall + face]
                if f % 2:
                    wl[f // 2] = wl[f // 2] + both[0:face]
            turned = corner_part(lambda f: ml[f])
        total(sy.at[it, pl.ds(0, nz - 1)], sy_send.at[it], sy_recv.at[it]).wait_recv()
        sums_now = jnp.sum(sy[it], axis=0)
        gamma, cross, delta = sums_now[0:1], sums_now[1:2], sums_now[2:3] + coarse_part
        if it == 0:
            curve = delta
        else:
            beta = gamma / gamma_old
            curve = delta + 2.0 * beta * cross + beta * beta * curve
        alpha = gamma / curve
        gamma_old = gamma

        if last:
            for a in range(3):
                r[a] = r[a] - alpha * (wl[a] + beta * s[a])
                x[a] = x[a] + alpha * (u[now, 2 * a + 1] + beta * p[a])
        else:
            cp_turned = turned if it == 0 else turned + beta * cp_turned
            cp = cp - alpha * cp_turned

    for copy in sent:
        copy.wait_send()
    total(idr.at[pl.ds(0, sz.lines - 1)], id_send, id_recv).wait_send()
    total(idz.at[pl.ds(0, nz - 1)], idz_send, idz_recv).wait_send()
    for it in range(ITERS):
        total(rxy.at[it, pl.ds(0, sz.lines - 1)], xy_send.at[it], xy_recv.at[it]).wait_send()
        total(sx.at[it, pl.ds(0, sz.lines - 1)], sx_send.at[it], sx_recv.at[it]).wait_send()
        total(sy.at[it, pl.ds(0, nz - 1)], sy_send.at[it], sy_recv.at[it]).wait_send()
        total(lev.at[it, 0, pl.ds(0, nz - 1)], z_send.at[it], z_recv.at[it]).wait_send()
        total(lev.at[it, 0], pp_send.at[it], pp_recv.at[it]).wait_send()
        part = hn.at[it, pl.ds(0, 3)] if it + 1 == ITERS else hn.at[it]
        total(part, h_send.at[it], h_recv.at[it]).wait_send()


def deliver(face, x, r, x_h, r_h, sem):
    outs = []
    for a in range(3):
        for n, (src, dst) in enumerate(((x, x_h), (r, r_h))):
            copy = pltpu.make_async_copy(src.at[a], dst.at[pl.ds(face * a, face), 0], sem.at[n, a])
            copy.start()
            outs.append(copy)
    for copy in outs:
        copy.wait()


def body(sz, dual_rhs, local_flex, corner_coupling, face_stiffness, coarse_inverse, corner_ids):
    nx, ny, nz = sz.grid
    face, dofs, cases = sz.face, sz.dofs, sz.cases
    vmem, dma = pltpu.VMEM, pltpu.SemaphoreType.DMA
    g_rows = 7 * 32
    it = ITERS
    scratch = [
        pltpu.SMEM((8,), jnp.int32), vmem((3, face, cases), F32), vmem((dofs, dofs), BF16), vmem((24, dofs), BF16),
        vmem((6, face, face), BF16), vmem((sz.coarse, sz.coarse), BF16),
        vmem((sz.block, sz.lines * 16), BF16), vmem((sz.names, sz.lines * 8), BF16), vmem((32, 24), BF16),
        vmem((3, face, cases), BF16), vmem((3, face, cases), BF16),
        vmem((3, face, cases), BF16), vmem((3, face, cases), BF16),
        vmem((6, face, sz.split), BF16), vmem((6, sz.rest, 128), BF16), vmem((6, sz.rest, 128), BF16),
        vmem((32, sz.wide), BF16), vmem((6, 32, face), BF16), vmem((6, 32, sz.window), BF16),
        vmem((sz.wide, 128), F32), vmem((sz.window, 128), F32), vmem((6, face, face), BF16),
        vmem((6, 2 * sz.tall, 128), BF16),
        vmem((3, face, cases), F32), vmem((6, face, cases), F32),
        vmem((2, 6, face, cases), F32), vmem((3, face, cases), F32),
        vmem((dofs, cases), F32), vmem((dofs, cases), BF16), vmem((dofs, cases), F32),
        vmem((3, face, cases), F32), vmem((6, face, cases), F32),
        vmem((it, 2, 16, cases), BF16), vmem((it, sz.lines, 16, cases), BF16),
        vmem((it, 2, nz, sz.block, cases), BF16), vmem((it, 6, face, cases), BF16),
        vmem((it, 6, face, cases), BF16), vmem((sz.rows, cases), BF16),
        vmem((sz.rows + g_rows, sz.rows), BF16), vmem((sz.rows, sz.coarse), BF16),
        vmem((sz.rows, sz.coarse), BF16),
        vmem((8, cases), BF16), vmem((sz.lines, 8, cases), BF16), vmem((nz, sz.names, cases), BF16),
        vmem((it, 2, 4, cases), F32), vmem((it, sz.lines, 4, cases), F32), vmem((it, nz, 4, cases), F32),
        dma((16,)), dma((24,)), dma((6,)), dma((6,)), dma((3,)), dma((3,)), dma((6,)),
        dma, dma, dma, dma,
    ] + [dma((it,)) for _ in range(12)]
    anywhere = pl.BlockSpec(memory_space=pl.ANY)
    whole = pl.BlockSpec(memory_space=pltpu.VMEM)
    held = pltpu.VMEM((3, face, cases), F32)
    out = jax.ShapeDtypeStruct((3 * face, 1, cases), F32)
    x, res = pl.pallas_call(
        functools.partial(kernel, sz),
        out_shape=(held, held),
        in_specs=[anywhere] * 9,
        out_specs=(whole, whole),
        scratch_shapes=scratch,
        compiler_params=pltpu.CompilerParams(
            collective_id=0, has_side_effects=True, vmem_limit_bytes=56 * 1024 * 1024
        ),
        name="dual_cg",
    )(
        corner_ids.reshape(8), dual_rhs.reshape(3 * face, 1, cases), local_flex.reshape(dofs, dofs),
        corner_coupling.reshape(24, dofs), face_stiffness.reshape(6, face, face), coarse_inverse,
        *(jnp.asarray(table, BF16) for table in (*plane_sums(sz), corner_order())),
    )
    x, res = pl.pallas_call(
        functools.partial(deliver, face),
        out_shape=(out, out),
        in_specs=[whole, whole],
        out_specs=(anywhere, anywhere),
        scratch_shapes=[dma((2, 3))],
        name="deliver",
    )(*(pltpu.with_memory_space_constraint(v, pltpu.VMEM) for v in (x, res)))
    shape = (1, 1, 1, 3, face, cases)
    return x.reshape(shape), res.reshape(shape)


def solution(mesh):
    grid = (mesh.shape["gx"], mesh.shape["gy"], mesh.shape["gz"])

    def run(dual_rhs, local_flex, corner_coupling, face_stiffness, coarse_inverse, corner_ids):
        sz = Sizes(grid, dual_rhs.shape[4], dual_rhs.shape[5], coarse_inverse.shape[0])
        deep = P("gx", "gy", "gz", None, None, None)
        mid = P("gx", "gy", "gz", None, None)
        return jax.shard_map(
            functools.partial(body, sz),
            mesh=mesh,
            in_specs=(deep, mid, mid, deep, P(), P("gx", "gy", "gz", None)),
            out_specs=(deep, deep),
            check_vma=False,
        )(dual_rhs, local_flex, corner_coupling, face_stiffness, coarse_inverse, corner_ids)

    return run
```
